64 devices in a mesh: dp: 4 (over x, y), cp: 16 (over z, core).
Axes of the slice: x: 2, y: 2, z: 8, core: 2. Of those that a mesh axis runs over, the one named last changes fastest.
The devices are a block of a 4x4x8 slice.
Arguments:
- hidden: bfloat16 [32768, 2304], P(('dp', 'cp')), parts along dimension 0
- w_query: bfloat16 [6, 2304, 8, 256], replicated
- w_key: bfloat16 [6, 2304, 4, 256], replicated
- w_value: bfloat16 [6, 2304, 4, 256], replicated
- w_out: bfloat16 [6, 8, 256, 2304], replicated
Outputs:
- output: bfloat16 [32768, 2304], P(('dp', 'cp')), parts along dimension 0
There are 4 independent parts. The reference program is written for one: setup_inputs(seed, part) draws one part's arguments, and reference() takes and returns one part's arrays. A program takes and returns all parts, laid end to end along the dimension named above; an argument that names none is the same for every part.
All inputs are finite; a program needn't handle non-finite values.
Results may differ from the reference program's by a relative error of at most 0.0115828.
Values are sent between devices in bfloat16 or wider.
A program may use at most 768 MiB of HBM per device.

```python
import jax
import jax.numpy as jnp
from jax import lax

TOK_DEV = 512
NUM_CP = 16
D = 2304
HEADS = 8
KV_HEADS = 4
HEAD = 256
WINDOW = 1024
LAYERS = 6

SEQ_LEN = TOK_DEV * NUM_CP
GROUP_SIZE = HEADS // KV_HEADS
QUERY_BLOCK = min(64, TOK_DEV)
NUM_BLOCKS = SEQ_LEN // QUERY_BLOCK
EPS_NORM = 1e-6
NEG_BIG = -1e30


def setup_inputs(seed: int = 0, part: int = 0) -> dict:
    base_key = jax.random.key(seed)
    hidden_key = jax.random.fold_in(jax.random.fold_in(base_key, 1), part)
    weight_keys = jax.random.split(jax.random.fold_in(base_key, 2), 4)
    hidden = jax.random.normal(hidden_key, (SEQ_LEN, D), jnp.float32)
    w_query = jax.random.normal(weight_keys[0], (LAYERS, D, HEADS, HEAD), jnp.float32) * D ** -0.5
    w_key = jax.random.normal(weight_keys[1], (LAYERS, D, KV_HEADS, HEAD), jnp.float32) * D ** -0.5
    w_value = jax.random.normal(weight_keys[2], (LAYERS, D, KV_HEADS, HEAD), jnp.float32) * D ** -0.5
    w_out = jax.random.normal(weight_keys[3], (LAYERS, HEADS, HEAD, D), jnp.float32) * (HEADS * HEAD) ** -0.5
    return {
        "hidden": hidden.astype(jnp.bfloat16),
        "w_query": w_query.astype(jnp.bfloat16),
        "w_key": w_key.astype(jnp.bfloat16),
        "w_value": w_value.astype(jnp.bfloat16),
        "w_out": w_out.astype(jnp.bfloat16),
    }


def rms_normed(rows_in):
    widened = rows_in.astype(jnp.float32)
    return widened * lax.rsqrt(jnp.mean(widened * widened, axis=-1, keepdims=True) + EPS_NORM)


def project(normed, weight):
    flat = weight.reshape(weight.shape[0], weight.shape[1] * weight.shape[2])
    product = jnp.dot(normed, flat, preferred_element_type=jnp.float32)
    return product.astype(jnp.bfloat16).reshape(normed.shape[0], weight.shape[1], weight.shape[2])


def attend_block(q_block, key_rows, value_rows, query_pos, key_pos, windowed):
    grouped = q_block.astype(jnp.float32).reshape(QUERY_BLOCK, KV_HEADS, GROUP_SIZE, HEAD)
    scores = jnp.einsum("qhgd,khd->hgqk", grouped, key_rows) * HEAD ** -0.5
    allowed = (key_pos[None, :] <= query_pos[:, None]) & (key_pos[None, :] >= 0)
    if windowed:
        allowed = allowed & (key_pos[None, :] > query_pos[:, None] - WINDOW)
    scores = jnp.where(allowed, scores, NEG_BIG)
    row_max = jnp.max(scores, axis=-1, keepdims=True)
    weights = jnp.exp(scores - row_max)
    row_sum = jnp.sum(weights, axis=-1)
    rounded = weights.astype(jnp.bfloat16).astype(jnp.float32)
    attn_out = jnp.einsum("hgqk,khd->hgqd", rounded, value_rows) / row_sum[..., None]
    return jnp.transpose(attn_out, (2, 0, 1, 3)).reshape(QUERY_BLOCK, HEADS, HEAD).astype(jnp.bfloat16)


def attention_layer(hidden, weights, windowed):
    w_query, w_key, w_value, w_out = weights
    normed = rms_normed(hidden).astype(jnp.bfloat16)
    queries = project(normed, w_query)
    key_rows = project(normed, w_key).astype(jnp.float32)
    value_rows = project(normed, w_value).astype(jnp.float32)
    if windowed:
        zero_pad = jnp.zeros((WINDOW, KV_HEADS, HEAD), jnp.float32)
        key_rows = jnp.concatenate([zero_pad, key_rows], axis=0)
        value_rows = jnp.concatenate([zero_pad, value_rows], axis=0)

    def one_block(block_idx):
        start_row = block_idx * QUERY_BLOCK
        q_block = lax.dynamic_slice_in_dim(queries, start_row, QUERY_BLOCK)
        query_pos = start_row + jnp.arange(QUERY_BLOCK)
        if windowed:
            key_span = WINDOW + QUERY_BLOCK
            key_blk = lax.dynamic_slice_in_dim(key_rows, start_row, key_span)
            value_blk = lax.dynamic_slice_in_dim(value_rows, start_row, key_span)
            key_pos = start_row - WINDOW + jnp.arange(key_span)
        else:
            key_blk = key_rows
            value_blk = value_rows
            key_pos = jnp.arange(SEQ_LEN)
        return attend_block(q_block, key_blk, value_blk, query_pos, key_pos, windowed)

    attn_out = lax.map(one_block, jnp.arange(NUM_BLOCKS)).reshape(SEQ_LEN, HEADS * HEAD)
    update = jnp.dot(attn_out, w_out.reshape(HEADS * HEAD, D), preferred_element_type=jnp.float32)
    return (hidden.astype(jnp.float32) + rms_normed(update)).astype(jnp.bfloat16)


def output_order(hidden):
    halves = hidden.reshape(2, NUM_CP, TOK_DEV // 2, D)
    return jnp.stack([halves[0], halves[1, ::-1]], axis=1).reshape(SEQ_LEN, D)


def reference(hidden, w_query, w_key, w_value, w_out):
    def local_step(state_in, weights):
        return attention_layer(state_in, weights, True), None

    stacked = (w_query[:LAYERS - 1], w_key[:LAYERS - 1], w_value[:LAYERS - 1], w_out[:LAYERS - 1])
    hidden = lax.scan(local_step, hidden, stacked)[0]
    last_weights = (w_query[LAYERS - 1], w_key[LAYERS - 1], w_value[LAYERS - 1], w_out[LAYERS - 1])
    hidden = attention_layer(hidden, last_weights, False)
    return output_order(hidden)
```

```python
import functools

import jax
import jax.numpy as jnp
from jax import lax
from jax.experimental import pallas as pl
from jax.experimental.pallas import tpu as pltpu
from jax.sharding import PartitionSpec as P

WINDOW = 1024
EPS_NORM = 1e-6
NEG_BIG = -1e30
LOG2_E = 1.4426950408889634
BLK = 256
VMEM_BYTES = 62 << 20


def params(**kw):
    return pltpu.CompilerParams(vmem_limit_bytes=VMEM_BYTES, **kw)


def normed(rows):
    wide = rows.astype(jnp.float32)
    return (wide * lax.rsqrt(jnp.mean(wide * wide, axis=-1, keepdims=True) + EPS_NORM)).astype(jnp.bfloat16)


def proj_kernel(layer, num_w, num_parts, *refs):
    x_ref, refs = refs[0], refs[1:]
    w_hbm, outs, n_s = refs[:num_w], refs[num_w:2 * num_w], refs[2 * num_w]
    stages, flats = refs[2 * num_w + 1:3 * num_w + 1], refs[3 * num_w + 1:4 * num_w + 1]
    sems = refs[-1]
    dim = x_ref.shape[1]
    part = dim // num_parts
    copies = []
    for i in range(num_w):
        row = []
        for p in range(num_parts):
            cp = pltpu.make_async_copy(w_hbm[i].at[layer, pl.ds(p * part, part)], stages[i].at[pl.ds(p * part, part)], sems.at[i, p])
            cp.start()
            row.append(cp)
        copies.append(row)
    n_s[...] = normed(x_ref[...])

    def flatten(i, start, size):
        rows = pl.ds(start, size)
        flats[i][rows, :] = stages[i][rows].reshape(size, -1)

    for p in range(num_parts):
        copies[0][p].wait()
        for b in range(0, part, BLK):
            flatten(0, p * part + b, BLK)
    for i in range(num_w):
        more = list(range(i + 1, num_w)) if i == 0 else []
        for j in more:
            for p in range(num_parts):
                copies[j][p].wait()
        width = flats[i].shape[1]
        tile = 512
        steps = width // tile
        rows = dim // steps

        @pl.loop(0, steps)
        def _(s):
            for j in more:
                flatten(j, pl.multiple_of(s * rows, 16), rows)
            cols = pl.ds(pl.multiple_of(s * tile, tile), tile)
            outs[i][:, cols] = jnp.dot(n_s[...], flats[i][:, cols], preferred_element_type=jnp.float32).astype(jnp.bfloat16)


def project(x, weights, layer):
    rows, dim = x.shape
    num_parts = 3
    shapes = [w.shape[2:] for w in weights]
    widths = [h * e for h, e in shapes]
    num_w = len(weights)
    vm = pl.BlockSpec(memory_space=pltpu.VMEM)
    flops = 2 * rows * dim * sum(widths)
    return pl.pallas_call(
        functools.partial(proj_kernel, layer, num_w, num_parts),
        in_specs=[vm] + [pl.BlockSpec(memory_space=pl.ANY)] * num_w,
        out_specs=[vm] * num_w,
        out_shape=[jax.ShapeDtypeStruct((rows, n), jnp.bfloat16) for n in widths],
        scratch_shapes=[pltpu.VMEM((rows, dim), jnp.bfloat16)]
        + [pltpu.VMEM((dim,) + s, jnp.bfloat16) for s in shapes]
        + [pltpu.VMEM((dim, n), jnp.bfloat16) for n in widths]
        + [pltpu.SemaphoreType.DMA((num_w, num_parts))],
        compiler_params=params(),
        cost_estimate=pl.CostEstimate(flops=flops, bytes_accessed=2 * dim * sum(widths), transcendentals=0),
        name=f"proj{num_w}",
    )(x, *weights)


def output_rows(o_s, w_s, x_ref, out_ref, upd_s):
    rows, dim = x_ref.shape
    tile = 768

    @pl.loop(0, dim // tile)
    def _(s):
        cols = pl.ds(pl.multiple_of(s * tile, tile), tile)
        upd_s[:, cols] = jnp.dot(o_s[...], w_s[:, cols], preferred_element_type=jnp.float32)

    @pl.loop(0, rows // 64)
    def _(s):
        part = pl.ds(pl.multiple_of(s * 64, 64), 64)
        upd = upd_s[part, :]
        scale = lax.rsqrt(jnp.mean(upd * upd, axis=-1, keepdims=True) + EPS_NORM)
        out_ref[part, :] = (x_ref[part, :].astype(jnp.float32) + upd * scale).astype(jnp.bfloat16)


def soft_block(q, keys, values, kinds):
    scores = []
    for k, kind in zip(keys, kinds):
        s = lax.dot_general(q, k, (((1,), (1,)), ((), ())), preferred_element_type=jnp.float32)
        if kind:
            qi = lax.broadcasted_iota(jnp.int32, s.shape, 0)
            ki = lax.broadcasted_iota(jnp.int32, s.shape, 1)
            s = jnp.where(ki <= qi if kind == 1 else ki > qi, s, NEG_BIG)
        scores.append(s)
    top = jnp.max(functools.reduce(jnp.maximum, scores), axis=-1, keepdims=True)
    factor = LOG2_E * q.shape[-1] ** -0.5
    acc = total = None
    for s, v in zip(scores, values):
        e = jnp.exp2((s - top) * factor)
        d = jnp.dot(e.astype(jnp.bfloat16), v, preferred_element_type=jnp.float32)
        total = e if total is None else total + e
        acc = d if acc is None else acc + d
    return (acc / jnp.sum(total, axis=-1, keepdims=True)).astype(jnp.bfloat16)


def window_kernel(layer, c_ref, q_ref, *refs):
    keys, values, (x_ref, w_hbm, out_ref, o_s, w_s, upd_s, sem) = refs[0:6:2], refs[1:6:2], refs[6:]
    g = pl.program_id(0)
    c = c_ref[0]
    wcopy = pltpu.make_async_copy(w_hbm.at[layer], w_s, sem)

    @pl.when(g == 0)
    def _():
        wcopy.start()

    def run(first_chunk):
        kinds = [-1, 0, 0, 0, 1]
        for i in range(2):
            picks = [(i + j, kinds[j]) for j in range(5) if (i + j) // 2 >= first_chunk]
            ks = [keys[b // 2][(b % 2) * BLK:(b % 2 + 1) * BLK, :] for b, _ in picks]
            vs = [values[b // 2][(b % 2) * BLK:(b % 2 + 1) * BLK, :] for b, _ in picks]
            for h in range(2):
                q = q_ref[i * BLK:(i + 1) * BLK, h * BLK:(h + 1) * BLK]
                res = soft_block(q, ks, vs, [kind for _, kind in picks])
                o_s[i * BLK:(i + 1) * BLK, pl.ds(pl.multiple_of(g * 2 * BLK + h * BLK, BLK), BLK)] = res

    for first, cond in ((0, c >= 2), (1, c == 1), (2, c == 0)):
        @pl.when(cond)
        def _():
            run(first)

    @pl.when(g == pl.num_programs(0) - 1)
    def _():
        wcopy.wait()
        output_rows(o_s, w_s, x_ref, out_ref, upd_s)


def window_layer(chunk, q, kvs, x, w_out, layer):
    rows, dim = x.shape
    kv = pl.BlockSpec((rows, BLK), lambda g, c: (0, g))
    row = pl.BlockSpec((rows, dim), lambda g, c: (0, 0))
    return pl.pallas_call(
        functools.partial(window_kernel, layer),
        grid_spec=pltpu.PrefetchScalarGridSpec(
            num_scalar_prefetch=1,
            grid=(kvs[0].shape[1] // BLK,),
            in_specs=[pl.BlockSpec((rows, 2 * BLK), lambda g, c: (0, g))] + [kv] * 6 + [row, pl.BlockSpec(memory_space=pl.ANY)],
            out_specs=row,
            scratch_shapes=[
                pltpu.VMEM(q.shape, jnp.bfloat16),
                pltpu.VMEM(w_out.shape[1:], jnp.bfloat16),
                pltpu.VMEM((rows, dim), jnp.float32),
                pltpu.SemaphoreType.DMA,
            ],
        ),
        out_shape=jax.ShapeDtypeStruct((rows, dim), jnp.bfloat16),
        compiler_params=params(),
        cost_estimate=pl.CostEstimate(flops=15 * 10 ** 9, bytes_accessed=2 * w_out[0].size, transcendentals=0),
        name="window",
    )(chunk, q, *kvs, x, w_out)


MESH = pl.DeviceIdType.MESH


def gather_kernel(num_dev, layer, shift, x_hbm, wk_hbm, wv_hbm, k_all, v_all, x_all,
                  wk_st, wv_st, wk_s, wv_s, x_s, n_s, k_s, v_s, wsem, lsem, ssem, send, recv, psend, precv):
    rows, dim = x_s.shape
    half = rows // 2
    me = lax.axis_index("cp")
    other = me + 1 - 2 * lax.rem(me, 2)
    near = (lax.rem(me + 2, num_dev), lax.rem(me + num_dev - 2, num_dev))
    hops = num_dev // 4

    def wrap(v):
        return lax.rem(v + 4 * num_dev, num_dev)

    def owner(dev, way, hop):
        return wrap(dev - 2 * hop) if way == 0 else wrap(dev + 2 * hop)

    def piece(dev, h):
        return x_all.at[dev, pl.ds(h * half, half)]

    def link(way, hop, h):
        ref = piece(owner(me, way, hop - 1), h)
        return pltpu.make_async_remote_copy(src_ref=ref, dst_ref=ref, send_sem=send.at[way, hop, h], recv_sem=recv.at[way, hop, h],
                                            device_id={"cp": near[way]}, device_id_type=MESH)

    def landed(way, hop, h):
        ref = piece(owner(me, way, hop), h)
        return pltpu.make_async_remote_copy(src_ref=ref, dst_ref=ref, send_sem=send.at[way, hop, h], recv_sem=recv.at[way, hop, h],
                                            device_id={"cp": near[way]}, device_id_type=MESH)

    def across(way, hop, h, dev):
        ref = piece(owner(dev, way, hop), h)
        return pltpu.make_async_remote_copy(src_ref=ref, dst_ref=ref, send_sem=psend.at[way, hop, h], recv_sem=precv.at[way, hop, h],
                                            device_id={"cp": other}, device_id_type=MESH)

    wcopies = [pltpu.make_async_copy(w.at[layer], st, wsem.at[i]) for i, (w, st) in enumerate(((wk_hbm, wk_st), (wv_hbm, wv_st)))]
    for cp in wcopies:
        cp.start()
    first = pltpu.make_async_copy(x_hbm, x_s, lsem)
    first.start()
    barrier = pltpu.get_barrier_semaphore()
    for dev in near + (other,):
        pl.semaphore_signal(barrier, inc=1, device_id={"cp": dev}, device_id_type=MESH)
    pl.semaphore_wait(barrier, 3)
    first.wait()
    keep = pltpu.make_async_copy(x_s, x_all.at[me], lsem)
    keep.start()
    keep.wait()
    for h in range(2):
        for way in range(2):
            link(way, 1, h).start()
    for h in range(2):
        across(0, 0, h, me).start()
    for cp in wcopies:
        cp.wait()
    step_rows = 256

    @pl.loop(0, dim // step_rows)
    def _(s):
        part = pl.ds(pl.multiple_of(s * step_rows, step_rows), step_rows)
        wk_s[part, :] = wk_st[part].reshape(step_rows, -1)
        wv_s[part, :] = wv_st[part].reshape(step_rows, -1)

    @pl.loop(0, hops + 1)
    def _(hop):
        for h in range(2):
            for way in range(2):
                last_ok = way == h

                def arrive():
                    landed(way, hop, h).wait_recv()
                    if last_ok:
                        @pl.when(hop < hops)
                        def _():
                            link(way, hop + 1, h).start()
                    else:
                        @pl.when(hop < hops - 1)
                        def _():
                            link(way, hop + 1, h).start()
                    across(way, hop, h, me).start()

                if last_ok:
                    pl.when(hop > 0)(arrive)
                else:
                    pl.when((hop > 0) & (hop < hops))(arrive)

        whole = (hop > 0) & (hop < hops)

        @pl.loop(0, 4)
        def _(a):
            way = lax.rem(a, 2)
            mine = a < 2

            @pl.when(whole | (way == 0))
            def _():
                @pl.when(jnp.logical_not(mine))
                def _():
                    for w in range(2):
                        for h in range(2):
                            pair = ((hop > 0) & (hop < hops) & (way == w))
                            if w == 0:
                                pair = pair | (hop == 0)
                            if w == h:
                                pair = pair | (hop == hops)

                            @pl.when(pair)
                            def _():
                                across(w, hop, h, other).wait_recv()

                dev = jnp.where(mine, me, other)
                src = wrap(dev + jnp.where(way == 0, -2, 2) * hop)
                load = pltpu.make_async_copy(x_all.at[src], x_s, lsem)
                load.start()
                load.wait()
                n_s[...] = normed(x_s[...])
                k_s[...] = jnp.dot(n_s[...], wk_s[...], preferred_element_type=jnp.float32).astype(jnp.bfloat16)
                v_s[...] = jnp.dot(n_s[...], wv_s[...], preferred_element_type=jnp.float32).astype(jnp.bfloat16)
                chunk = wrap(src + shift)
                stores = [pltpu.make_async_copy(s, o.at[chunk], ssem.at[i]) for i, (s, o) in enumerate(((k_s, k_all), (v_s, v_all)))]
                for cp in stores:
                    cp.start()
                for cp in stores:
                    cp.wait()

    for way in range(2):
        for hop in range(1, hops + 1):
            for h in range(2):
                if hop < hops or way == h:
                    link(way, hop, h).wait_send()
                    across(way, hop, h, me).wait_send()
    for h in range(2):
        across(0, 0, h, me).wait_send()


def gather_keys(x, w_key, w_value, layer, shift, num_dev):
    rows, dim = x.shape
    heads, head_dim = w_key.shape[2:]
    width = heads * head_dim
    hops = num_dev // 4
    any_ = pl.BlockSpec(memory_space=pl.ANY)
    bf = jnp.bfloat16
    sem = pltpu.SemaphoreType.DMA
    return pl.pallas_call(
        functools.partial(gather_kernel, num_dev, layer, shift),
        in_specs=[any_] * 3,
        out_specs=[any_] * 3,
        out_shape=[jax.ShapeDtypeStruct((num_dev, rows, n), bf) for n in (width, width, dim)],
        scratch_shapes=[pltpu.VMEM((dim, heads, head_dim), bf)] * 2 + [pltpu.VMEM((dim, width), bf)] * 2
        + [pltpu.VMEM((rows, dim), bf)] * 2 + [pltpu.VMEM((rows, width), bf)] * 2
        + [sem((2,)), sem, sem((2,))] + [sem((2, hops + 1, 2))] * 4,
        compiler_params=params(collective_id=1, has_side_effects=True),
        cost_estimate=pl.CostEstimate(flops=4 * rows * num_dev * dim * width, bytes_accessed=4 * dim * width, transcendentals=0),
        name="gather",
    )(x, w_key, w_value)


def causal_kernel(layer, seq, blk_ref, q_ref, k_ref, v_ref, x_ref, w_hbm, out_ref, o_s, w_s, upd_s, acc_s, top_s, tot_s, sem):
    g = pl.program_id(0)
    wcopy = pltpu.make_async_copy(w_hbm.at[layer], w_s, sem)

    @pl.when(g == 0)
    def _():
        wcopy.start()

    lead, trail = blk_ref[0], blk_ref[1]
    tile = 4 * BLK
    lanes = tot_s.shape[-1]
    per = tile // BLK
    front = seq // 2 // tile
    num_trail = lax.div(trail + 1 + per - 1, per) - front
    num_lead = lax.div(lead + 1 + per - 1, per)
    factor = LOG2_E * BLK ** -0.5
    acc_s[...] = jnp.zeros_like(acc_s)
    tot_s[...] = jnp.zeros_like(tot_s)
    top_s[...] = jnp.full_like(top_s, NEG_BIG)

    def update(chains):
        scores = []
        for slot, qrow, t, limit in chains:
            rows = pl.ds(pl.multiple_of(t * tile, tile), tile)
            for h in range(2):
                q = q_ref[pl.ds(qrow, BLK), h * BLK:(h + 1) * BLK]
                s = lax.dot_general(q, k_ref[rows, :], (((1,), (1,)), ((), ())), preferred_element_type=jnp.float32)
                if limit is not None:
                    ahead = lax.broadcasted_iota(jnp.int32, s.shape, 1) - lax.broadcasted_iota(jnp.int32, s.shape, 0)
                    s = jnp.where(ahead <= limit, s, NEG_BIG)
                scores.append((s, slot, h, rows))
        for s, slot, h, rows in scores:
            top = top_s[slot, h]
            new = jnp.maximum(top, jnp.max(s, axis=-1, keepdims=True))
            fix = jnp.exp2((top - new) * factor)
            e = jnp.exp2((s - new) * factor)
            part = functools.reduce(jnp.add, [e[:, i * lanes:(i + 1) * lanes] for i in range(tile // lanes)])
            tot_s[slot, h] = tot_s[slot, h] * fix + part
            acc_s[slot, h] = acc_s[slot, h] * fix + jnp.dot(e.astype(jnp.bfloat16), v_ref[rows, :], preferred_element_type=jnp.float32)
            top_s[slot, h] = new

    def second(j):
        late = j < num_trail
        t = jnp.where(late, front + j, j - num_trail)
        limit = jnp.where(late, trail, lead) * BLK - t * tile
        return jnp.where(late, 1, 2), pl.multiple_of(jnp.where(late, BLK, 0), BLK), t, limit

    @pl.loop(0, front)
    def _(j):
        update([(0, BLK, j, None), second(j)])

    @pl.loop(front, num_trail + num_lead)
    def _(j):
        update([second(j)])

    for h in range(2):
        cols = pl.ds(pl.multiple_of(g * 2 * BLK + h * BLK, BLK), BLK)
        new = jnp.maximum(top_s[0, h], top_s[1, h])
        fixes = [jnp.exp2((top_s[i, h] - new) * factor) for i in range(2)]
        total = jnp.sum(tot_s[0, h] * fixes[0] + tot_s[1, h] * fixes[1], axis=-1, keepdims=True)
        o_s[BLK:, cols] = ((acc_s[0, h] * fixes[0] + acc_s[1, h] * fixes[1]) / total).astype(jnp.bfloat16)
        o_s[:BLK, cols] = (acc_s[2, h] / jnp.sum(tot_s[2, h], axis=-1, keepdims=True)).astype(jnp.bfloat16)

    @pl.when(g == pl.num_programs(0) - 1)
    def _():
        wcopy.wait()
        output_rows(o_s, w_s, x_ref, out_ref, upd_s)


def causal_layer(blocks, q, k_all, v_all, x, w_out, layer):
    rows, dim = x.shape
    seq = k_all.shape[0]
    kv = pl.BlockSpec((seq, BLK), lambda g, b: (0, g))
    row = pl.BlockSpec((rows, dim), lambda g, b: (0, 0))
    return pl.pallas_call(
        functools.partial(causal_kernel, layer, seq),
        grid_spec=pltpu.PrefetchScalarGridSpec(
            num_scalar_prefetch=1,
            grid=(k_all.shape[1] // BLK,),
            in_specs=[pl.BlockSpec((rows, 2 * BLK), lambda g, b: (0, g)), kv, kv, row, pl.BlockSpec(memory_space=pl.ANY)],
            out_specs=row,
            scratch_shapes=[
                pltpu.VMEM(q.shape, jnp.bfloat16),
                pltpu.VMEM(w_out.shape[1:], jnp.bfloat16),
                pltpu.VMEM((rows, dim), jnp.float32),
                pltpu.VMEM((3, 2, BLK, BLK), jnp.float32),
                pltpu.VMEM((3, 2, BLK, 1), jnp.float32),
                pltpu.VMEM((3, 2, BLK, 128), jnp.float32),
                pltpu.SemaphoreType.DMA,
            ],
        ),
        out_shape=jax.ShapeDtypeStruct((rows, dim), jnp.bfloat16),
        compiler_params=params(),
        cost_estimate=pl.CostEstimate(flops=30 * 10 ** 9, bytes_accessed=2 * w_out[0].size, transcendentals=0),
        name="causal",
    )(blocks, q, k_all, v_all, x, w_out)


def solution(mesh):
    num_dev = mesh.shape["cp"]

    def ring(hop):
        return [(i, (i + hop) % num_dev) for i in range(num_dev)]

    def per_device(hidden, w_query, w_key, w_value, w_out):
        rank = lax.axis_index("cp")
        num_layers = w_query.shape[0]
        rows, dim = hidden.shape
        w_out = w_out.reshape(num_layers, -1, dim)
        last = num_layers - 1
        x = hidden
        for layer in range(last):
            chunk = lax.rem(rank + layer + 1, num_dev).astype(jnp.int32).reshape(1)
            x_next = lax.ppermute(x, "cp", ring(-1))
            k_own, v_own = project(x, (w_key, w_value), layer)
            k_halo = lax.ppermute(k_own, "cp", ring(1))
            v_halo = lax.ppermute(v_own, "cp", ring(1))
            q, k_cur, v_cur = project(x_next, (w_query, w_key, w_value), layer)
            x = window_layer(chunk, q, (k_halo, v_halo, k_own, v_own, k_cur, v_cur), x_next, w_out, layer)

        k_all, v_all, x_all = gather_keys(x, w_key, w_value, last, last, num_dev)
        half = rows // 2
        blocks = jnp.stack([rank, 2 * num_dev - 1 - rank]).astype(jnp.int32)
        rows_fin = []
        for i in range(2):
            owner = lax.rem(blocks[i] // 2 - last + num_dev, num_dev)
            rows_fin.append(lax.dynamic_slice(x_all, (owner, lax.rem(blocks[i], 2) * half, jnp.int32(0)), (1, half, dim)).reshape(half, dim))
        x_fin = jnp.concatenate(rows_fin, axis=0)
        q, = project(x_fin, (w_query,), last)
        return causal_layer(blocks, q, k_all.reshape(-1, k_all.shape[-1]), v_all.reshape(-1, v_all.shape[-1]), x_fin, w_out, last)

    row_spec = P(("dp", "cp"), None)
    return jax.shard_map(per_device, mesh=mesh, in_specs=(row_spec, P(), P(), P(), P()), out_specs=row_spec, check_vma=False)
```

```python
import functools

import jax
import jax.numpy as jnp
from jax import lax
from jax.experimental import pallas as pl
from jax.experimental.pallas import tpu as pltpu
from jax.sharding import PartitionSpec as P

WINDOW = 1024
EPS_NORM = 1e-6
NEG_BIG = -1e30
LOG2_E = 1.4426950408889634
BLK = 256
VMEM_BYTES = 62 << 20
MESH = pl.DeviceIdType.MESH


def params(**kw):
    return pltpu.CompilerParams(vmem_limit_bytes=VMEM_BYTES, **kw)


def normed(rows):
    wide = rows.astype(jnp.float32)
    return (wide * lax.rsqrt(jnp.mean(wide * wide, axis=-1, keepdims=True) + EPS_NORM)).astype(jnp.bfloat16)


def output_rows(o_s, w_s, x_ref, out_ref, upd_s):
    rows, dim = x_ref.shape
    tile = 768

    @pl.loop(0, dim // tile)
    def _(s):
        cols = pl.ds(pl.multiple_of(s * tile, tile), tile)
        upd_s[:, cols] = jnp.dot(o_s[...], w_s[:, cols], preferred_element_type=jnp.float32)

    @pl.loop(0, rows // 64)
    def _(s):
        part = pl.ds(pl.multiple_of(s * 64, 64), 64)
        upd = upd_s[part, :]
        scale = lax.rsqrt(jnp.mean(upd * upd, axis=-1, keepdims=True) + EPS_NORM)
        out_ref[part, :] = (x_ref[part, :].astype(jnp.float32) + upd * scale).astype(jnp.bfloat16)


def scoped(name):
    def wrap(fn):
        def run(*args):
            with jax.named_scope(name):
                return fn(*args)

        return run

    return wrap


def stack_kernel(num_dev, num_layers, x_hbm, wq_hbm, wk_hbm, wv_hbm, wo_hbm, out_hbm,
                 xr, xn, kv, n_s, q_s, wq_s, wkv_s, wo_s, upd_s, stq, stk, stv,
                 x_send, x_recv, h_send, h_recv, c_send, c_recv, h_free, c_free, xsem, qsem, ksem, vsem, wsem):
    blk, dim = n_s.shape
    width = wkv_s.shape[1] // 2
    heads = q_s.shape[2] // width
    head = BLK
    q_rows, kv_rows = stq.shape[1], stk.shape[1]
    q_ring, kv_ring = stq.shape[0], stk.shape[0]
    q_parts, kv_parts = dim // q_rows, dim // kv_rows
    me = lax.axis_index("cp")
    odd = lax.rem(me, 2)
    is_odd, is_even = odd == 1, odd == 0
    left, right = lax.rem(me + num_dev - 1, num_dev), lax.rem(me + 1, num_dev)

    def block(i):
        return pl.ds(pl.multiple_of(i * blk, blk), blk)

    def remote(src, dst, send, recv, dev):
        return pltpu.make_async_remote_copy(src_ref=src, dst_ref=dst, send_sem=send, recv_sem=recv, device_id={"cp": dev}, device_id_type=MESH)

    def x_copy(slot, s):
        return remote(xn.at[s], xr.at[slot, s], x_send.at[s], x_recv.at[slot, s], left)

    def h_copy(s):
        return remote(kv.at[block(2 + s)], kv.at[block(s)], h_send.at[s], h_recv.at[s], right)

    def c_copy(s):
        return remote(kv.at[block(2 + s)], kv.at[block(4 + s)], c_send.at[s], c_recv.at[s], left)

    def signal(sem, dev):
        pl.semaphore_signal(sem, inc=1, device_id={"cp": dev}, device_id_type=MESH)

    def q_stage(layer, i):
        b = lax.rem(layer * q_parts + i, q_ring)
        return pltpu.make_async_copy(wq_hbm.at[layer, pl.ds(i * q_rows, q_rows)], stq.at[b], qsem.at[b])

    def kv_stage(layer, i):
        b = lax.rem(layer * kv_parts + i, kv_ring)
        rows = pl.ds(i * kv_rows, kv_rows)
        return (pltpu.make_async_copy(wk_hbm.at[layer, rows], stk.at[b], ksem.at[b]),
                pltpu.make_async_copy(wv_hbm.at[layer, rows], stv.at[b], vsem.at[b]))

    def kv_start(layer, i):
        for cp in kv_stage(layer, i):
            cp.start()

    def kv_wait(layer, i):
        for cp in kv_stage(layer, i):
            cp.wait()

    def kv_flat(layer, i):
        b = lax.rem(layer * kv_parts + i, kv_ring)
        rows = pl.ds(pl.multiple_of(i * kv_rows, 16), kv_rows)
        wkv_s[rows, :width] = stk[b].reshape(kv_rows, width)
        wkv_s[rows, width:] = stv[b].reshape(kv_rows, width)

    def q_flat(layer, i):
        b = lax.rem(layer * q_parts + i, q_ring)
        wq_s[pl.ds(pl.multiple_of(i * q_rows, 16), q_rows), :] = stq[b].reshape(q_rows, wq_s.shape[1])

    def kv_next(layer, i):
        @pl.when(i + kv_ring < kv_parts)
        def _():
            kv_start(layer, i + kv_ring)

    def q_next(layer, i):
        after = i + q_ring

        @pl.when(after < q_parts)
        def _():
            q_stage(layer, after).start()

        @pl.when((after >= q_parts) & (layer + 1 < num_layers))
        def _():
            q_stage(layer + 1, after - q_parts).start()

    def wo_copy(layer):
        return pltpu.make_async_copy(wo_hbm.at[layer], wo_s, wsem)

    def norm_into(ref):
        step = min(64, blk)

        @pl.loop(0, blk // step)
        def _(i):
            part = pl.ds(pl.multiple_of(i * step, step), step)
            n_s[part, :] = normed(ref[part, :])

    def dot(w):
        return jnp.dot(n_s[...], w, preferred_element_type=jnp.float32).astype(jnp.bfloat16)

    def attend(s, span, start):
        window = WINDOW + blk
        rows = pl.ds(pl.multiple_of(s * blk + window - span, blk), span)
        factor = LOG2_E * head ** -0.5
        groups = width // head
        together = groups if span == window else 2
        qi = lax.broadcasted_iota(jnp.int32, (blk, blk), 0)
        ki = lax.broadcasted_iota(jnp.int32, (blk, blk), 1)

        def scores(item):
            sc = lax.dot_general(q_s[s, :, item[2]], kv[rows, item[0]], (((1,), (1,)), ((), ())), preferred_element_type=jnp.float32)
            last = jnp.where(ki <= qi, sc[:, span - blk:], NEG_BIG)
            if span == window:
                return jnp.concatenate([jnp.where(ki > qi, sc[:, :blk], NEG_BIG), sc[:, blk:span - blk], last], axis=1)
            mid = sc[:, :span - blk]
            pos = lax.broadcasted_iota(jnp.int32, mid.shape, 1)
            return jnp.concatenate([jnp.where(pos >= start - (window - span), mid, NEG_BIG), last], axis=1)

        def finish(sc, item):
            top = jnp.max(sc, axis=-1, keepdims=True)
            e = jnp.exp2((sc - top) * factor)
            total = jnp.sum(e, axis=-1, keepdims=True)
            acc = jnp.dot(e.astype(jnp.bfloat16), kv[rows, item[1]], preferred_element_type=jnp.float32)
            return (acc / total).astype(jnp.bfloat16)

        def some(first):
            items = []
            for u in range(together):
                g = first + u
                for h in range(heads):
                    offsets = (g * head, width + g * head, (g * heads + h) * head)
                    items.append(tuple(pl.ds(o if isinstance(o, int) else pl.multiple_of(o, head), head) for o in offsets))
            ahead = scores(items[0])
            for k, item in enumerate(items):
                now = ahead
                if k + 1 < len(items):
                    ahead = scores(items[k + 1])
                q_s[s, :, item[2]] = finish(now, item)

        if together == groups:
            some(0)
        else:
            @pl.loop(0, groups // together)
            def _(i):
                some(i * together)

    tile = width
    loads = [pltpu.make_async_copy(x_hbm.at[block(s)], xn.at[s], xsem.at[s]) for s in range(2)]
    for cp in loads:
        cp.start()
    for i in range(kv_ring):
        kv_start(0, i)
    for i in range(q_ring):
        q_stage(0, i).start()
    barrier = pltpu.get_barrier_semaphore()
    for dev in (left, right):
        signal(barrier, dev)
    pl.semaphore_wait(barrier, 2)
    for s in range(2):
        loads[s].wait()
        x_copy(0, s).start()

    @pl.loop(0, kv_parts)
    def _(i):
        kv_wait(0, i)
        kv_flat(0, i)
        kv_next(0, i)

    @pl.loop(0, num_layers)
    def _(layer):
        slot = lax.rem(layer, 2)
        more = layer + 1 < num_layers
        chunk = lax.rem(me + layer + 1, num_dev)

        @pl.when(layer > 0)
        def _():
            for s in range(2):
                h_copy(s).wait_send()

            @pl.when(is_odd)
            def _():
                for s in range(2):
                    c_copy(s).wait_send()

        @pl.loop(0, 2)
        def _(s):
            with jax.named_scope("own_norm"):
                norm_into(xn.at[s])

            @pl.loop(0, 2)
            @scoped("own")
            def _(j):
                per = q_parts // 4
                first = (2 * s + j) * per
                for t in range(per):
                    q_stage(layer, first + t).wait()
                    q_flat(layer, first + t)
                    q_next(layer, first + t)
                cols = pl.ds(pl.multiple_of(j * tile, tile), tile)
                kv[block(2 + s), cols] = dot(wkv_s[:, cols])

            @pl.when((layer > 0) & (s == 0))
            @scoped("credit")
            def _():
                pl.semaphore_wait(h_free, 1)

                @pl.when(is_odd)
                def _():
                    pl.semaphore_wait(c_free, 1)

            h_copy(s).start()

            @pl.when(is_odd)
            def _():
                c_copy(s).start()

        wo_copy(layer).start()

        @pl.when(more)
        def _():
            for i in range(kv_ring):
                kv_start(layer + 1, i)

        @pl.loop(0, 2)
        def _(s):
            @pl.loop(jnp.where(is_odd, s, 2 * s), jnp.where(is_odd, s + 1, 2))
            def _(t):
                with jax.named_scope("x_wait"):
                    x_copy(slot, t).wait_recv()
                with jax.named_scope("norm"):
                    norm_into(xr.at[slot, t])

                @pl.loop(0, 2)
                @scoped("query")
                def _(j):
                    cols = pl.ds(pl.multiple_of(j * tile, tile), tile)
                    q_s[t, :, cols] = dot(wq_s[:, cols])

                @pl.when(is_odd)
                def _():
                    @pl.loop(0, 2)
                    @scoped("keys")
                    def _(j):
                        cols = pl.ds(pl.multiple_of(j * tile, tile), tile)
                        kv[block(4 + t), cols] = dot(wkv_s[:, cols])

            @pl.when(s == 0)
            @scoped("h_wait")
            def _():
                for i in range(2):
                    h_copy(i).wait_recv()

            @pl.when(is_even)
            @scoped("c_wait")
            def _():
                c_copy(s).wait_recv()

            for first, cond in ((2, chunk >= 2), (1, chunk == 1), (0, chunk == 0)):
                @pl.when(cond)
                @scoped("attend")
                def _():
                    attend(s, (2 * first + 1) * blk if first == 2 else (2 * first + 2) * blk, WINDOW - s * blk - first * 2 * blk)

            @pl.when((s == 1) & more)
            def _():
                signal(h_free, left)

                @pl.when(is_even)
                def _():
                    signal(c_free, right)

            out_tiles = 3
            out_tile = dim // out_tiles

            @pl.when(s == 0)
            def _():
                wo_copy(layer).wait()

            def out_dot(j):
                cols = pl.ds(pl.multiple_of(j * out_tile, out_tile), out_tile)
                upd_s[:, cols] = jnp.dot(q_s[s], wo_s[:, cols], preferred_element_type=jnp.float32)

            relay = (s == 1) & more

            @pl.when(relay)
            def _():
                @pl.loop(0, out_tiles)
                @scoped("out_lay")
                def _(j):
                    per = kv_parts // out_tiles
                    for t in range(per):
                        kv_wait(layer + 1, j * per + t)
                        kv_flat(layer + 1, j * per + t)
                        kv_next(layer + 1, j * per + t)
                    out_dot(j)

            @pl.when(jnp.logical_not(relay))
            def _():
                @pl.loop(0, out_tiles)
                @scoped("out")
                def _(j):
                    out_dot(j)

            with jax.named_scope("x_sent"):
                x_copy(slot, s).wait_send()
            step = min(64, blk)

            @pl.loop(0, blk // step)
            @scoped("resid")
            def _(i):
                part = pl.ds(pl.multiple_of(i * step, step), step)
                upd = upd_s[part, :]
                scale = lax.rsqrt(jnp.mean(upd * upd, axis=-1, keepdims=True) + EPS_NORM)
                xn[s, part, :] = (xr[slot, s, part, :].astype(jnp.float32) + upd * scale).astype(jnp.bfloat16)

            @pl.when(more)
            def _():
                x_copy(1 - slot, s).start()

            @pl.when(jnp.logical_not(more))
            def _():
                pltpu.make_async_copy(xn.at[s], out_hbm.at[block(s)], xsem.at[s]).start()

    for s in range(2):
        h_copy(s).wait_send()
        pltpu.make_async_copy(xn.at[s], out_hbm.at[block(s)], xsem.at[s]).wait()

    @pl.when(is_odd)
    def _():
        for s in range(2):
            c_copy(s).wait_send()


def window_stack(x, w_query, w_key, w_value, w_out, num_layers, num_dev):
    rows, dim = x.shape
    blk = rows // 2
    q_heads, head = w_query.shape[2:]
    kv_heads = w_key.shape[2]
    q_width, width = q_heads * head, kv_heads * head
    q_rows, q_ring, kv_rows, kv_ring = dim // 8, 3, dim // 9, 4
    any_ = pl.BlockSpec(memory_space=pl.ANY)
    bf = jnp.bfloat16
    dma, regular = pltpu.SemaphoreType.DMA, pltpu.SemaphoreType.REGULAR
    return pl.pallas_call(
        functools.partial(stack_kernel, num_dev, num_layers),
        in_specs=[any_] * 5,
        out_specs=any_,
        out_shape=jax.ShapeDtypeStruct((rows, dim), bf),
        scratch_shapes=[
            pltpu.VMEM((2, 2, blk, dim), bf),
            pltpu.VMEM((2, blk, dim), bf),
            pltpu.VMEM((6 * blk, 2 * width), bf),
            pltpu.VMEM((blk, dim), bf),
            pltpu.VMEM((2, blk, q_width), bf),
            pltpu.VMEM((dim, q_width), bf),
            pltpu.VMEM((dim, 2 * width), bf),
            pltpu.VMEM((q_width, dim), bf),
            pltpu.VMEM((blk, dim), jnp.float32),
            pltpu.VMEM((q_ring, q_rows, q_heads, head), bf),
            pltpu.VMEM((kv_ring, kv_rows, kv_heads, head), bf),
            pltpu.VMEM((kv_ring, kv_rows, kv_heads, head), bf),
            dma((2,)), dma((2, 2)), dma((2,)), dma((2,)), dma((2,)), dma((2,)),
            regular, regular, dma((2,)), dma((q_ring,)), dma((kv_ring,)), dma((kv_ring,)), dma,
        ],
        compiler_params=pltpu.CompilerParams(vmem_limit_bytes=67043328, collective_id=2, has_side_effects=True),
        cost_estimate=pl.CostEstimate(flops=num_layers * 20 * 10 ** 9, bytes_accessed=num_layers * 28 * 10 ** 6, transcendentals=0),
        name="stack",
    )(x, w_query, w_key, w_value, w_out)


def norm_rows(src, dst):
    rows = src.shape[0]
    step = min(64, rows)

    @pl.loop(0, rows // step)
    def _(i):
        part = pl.ds(pl.multiple_of(i * step, step), step)
        dst[part, :] = normed(src[part, :])


def gather_kernel(num_dev, layer, shift, x_hbm, wq_hbm, wk_hbm, wv_hbm, k_all, v_all, x_all, q_hbm, x_fin,
                  wq_st, wk_st, wv_st, wq_s, wk_s, wv_s, x_s, n_s, k_s, v_s, q_s, wsem, lsem, ssem, send, recv, psend, precv):
    _, rows, dim = x_s.shape
    half = rows // 2
    me = lax.axis_index("cp")
    other = me + 1 - 2 * lax.rem(me, 2)
    near = (lax.rem(me + 2, num_dev), lax.rem(me + num_dev - 2, num_dev))
    hops = num_dev // 4

    def wrap(v):
        return lax.rem(v + 4 * num_dev, num_dev)

    def owner(dev, way, hop):
        if isinstance(way, int):
            return wrap(dev - 2 * hop) if way == 0 else wrap(dev + 2 * hop)
        return wrap(dev + jnp.where(way == 0, -2, 2) * hop)

    def piece(dev, h):
        return x_all.at[dev, pl.ds(h * half, half)]

    def link(way, hop, h):
        ref = piece(owner(me, way, hop - 1), h)
        src = x_hbm.at[pl.ds(h * half, half)] if isinstance(hop, int) and hop == 1 else ref
        return pltpu.make_async_remote_copy(src_ref=src, dst_ref=ref, send_sem=send.at[way, hop, h], recv_sem=recv.at[way, hop, h],
                                            device_id={"cp": near[way]}, device_id_type=MESH)

    def landed(way, hop, h):
        ref = piece(owner(me, way, hop), h)
        return pltpu.make_async_remote_copy(src_ref=ref, dst_ref=ref, send_sem=send.at[way, hop, h], recv_sem=recv.at[way, hop, h],
                                            device_id={"cp": near[way]}, device_id_type=MESH)

    def across(way, hop, h, dev):
        ref = piece(owner(dev, way, hop), h)
        src = x_hbm.at[pl.ds(h * half, half)] if isinstance(hop, int) and hop == 0 else ref
        return pltpu.make_async_remote_copy(src_ref=src, dst_ref=ref, send_sem=psend.at[way, hop, h], recv_sem=precv.at[way, hop, h],
                                            device_id={"cp": other}, device_id_type=MESH)

    wcopies = [pltpu.make_async_copy(w.at[layer], st, wsem.at[i]) for i, (w, st) in enumerate(((wk_hbm, wk_st), (wv_hbm, wv_st), (wq_hbm, wq_st)))]
    for cp in wcopies:
        cp.start()
    first = pltpu.make_async_copy(x_hbm, x_s.at[0], lsem.at[0])
    first.start()
    barrier = pltpu.get_barrier_semaphore()
    for dev in near + (other,):
        pl.semaphore_signal(barrier, inc=1, device_id={"cp": dev}, device_id_type=MESH)
    pl.semaphore_wait(barrier, 3)
    for h in range(2):
        for way in range(2):
            link(way, 1, h).start()
    for h in range(2):
        across(0, 0, h, me).start()
    first.wait()
    keep = pltpu.make_async_copy(x_s.at[0], x_all.at[me], lsem.at[0])
    keep.start()
    keep.wait()
    for cp in wcopies:
        cp.wait()
    step_rows = 256

    @pl.loop(0, dim // step_rows)
    def _(s):
        part = pl.ds(pl.multiple_of(s * step_rows, step_rows), step_rows)
        wk_s[part, :] = wk_st[part].reshape(step_rows, -1)
        wv_s[part, :] = wv_st[part].reshape(step_rows, -1)
        wq_s[part, :] = wq_st[part].reshape(step_rows, -1)

    @pl.loop(0, hops + 1)
    def _(hop):
        for h in range(2):
            for way in range(2):
                last_ok = way == h

                def arrive():
                    with jax.named_scope("land"):
                        landed(way, hop, h).wait_recv()
                    if last_ok:
                        @pl.when(hop < hops)
                        def _():
                            link(way, hop + 1, h).start()
                    else:
                        @pl.when(hop < hops - 1)
                        def _():
                            link(way, hop + 1, h).start()
                    across(way, hop, h, me).start()

                if last_ok:
                    pl.when(hop > 0)(arrive)
                else:
                    pl.when((hop > 0) & (hop < hops))(arrive)

        whole = (hop > 0) & (hop < hops)
        count = jnp.where(whole, 4, 2)

        def source(a):
            mine = a < lax.div(count, 2)
            way = jnp.where(whole, lax.rem(a, 2), 0)
            return mine, way, wrap(jnp.where(mine, me, other) + jnp.where(way == 0, -2, 2) * hop)

        def load(a):
            b = lax.rem(a, 2)
            return pltpu.make_async_copy(x_all.at[source(a)[2]], x_s.at[b], lsem.at[b])

        def stores(a):
            b = lax.rem(a, 2)
            chunk = wrap(source(a)[2] + shift)
            return [pltpu.make_async_copy(t.at[b], o.at[chunk], ssem.at[i, b]) for i, (t, o) in enumerate(((k_s, k_all), (v_s, v_all)))]

        def fetch(a):
            mine, way, _ = source(a)

            @pl.when(jnp.logical_not(mine))
            @scoped("cross")
            def _():
                for h in range(2):
                    across(jnp.where(hop == hops, h, way), hop, h, other).wait_recv()

            load(a).start()

        fetch(0)

        @pl.loop(0, count)
        def _(a):
            b = lax.rem(a, 2)

            @pl.when(a + 1 < count)
            def _():
                fetch(a + 1)

            with jax.named_scope("load"):
                load(a).wait()
            with jax.named_scope("norm"):
                norm_rows(x_s.at[b], n_s)

            @pl.when(a >= 2)
            @scoped("store")
            def _():
                for cp in stores(a - 2):
                    cp.wait()

            with jax.named_scope("keys"):
                k_s[b] = jnp.dot(n_s[...], wk_s[...], preferred_element_type=jnp.float32).astype(jnp.bfloat16)
                v_s[b] = jnp.dot(n_s[...], wv_s[...], preferred_element_type=jnp.float32).astype(jnp.bfloat16)
            for cp in stores(a):
                cp.start()

        for back in range(2):
            for cp in stores(count - 2 + back):
                cp.wait()

    loads = []
    for i, block in enumerate((me, 2 * num_dev - 1 - me)):
        src = wrap(lax.div(block, 2) - shift)
        loads.append(pltpu.make_async_copy(piece(src, lax.rem(block, 2)), x_s.at[0, pl.ds(i * half, half)], lsem.at[i]))
        loads[i].start()
    for cp in loads:
        cp.wait()
    keep = pltpu.make_async_copy(x_s.at[0], x_fin, lsem.at[0])
    keep.start()
    norm_rows(x_s.at[0], n_s)
    with jax.named_scope("query"):
        q_s[...] = jnp.dot(n_s[...], wq_s[...], preferred_element_type=jnp.float32).astype(jnp.bfloat16)
    last = pltpu.make_async_copy(q_s, q_hbm, lsem.at[1])
    last.start()
    last.wait()
    keep.wait()
    for way in range(2):
        for hop in range(1, hops + 1):
            for h in range(2):
                if hop < hops or way == h:
                    link(way, hop, h).wait_send()
                    across(way, hop, h, me).wait_send()
    for h in range(2):
        across(0, 0, h, me).wait_send()


def gather_keys(x, w_query, w_key, w_value, layer, shift, num_dev):
    rows, dim = x.shape
    shapes = [w.shape[2:] for w in (w_query, w_key, w_value)]
    q_width, width = (h * e for h, e in shapes[:2])
    hops = num_dev // 4
    any_ = pl.BlockSpec(memory_space=pl.ANY)
    bf = jnp.bfloat16
    sem = pltpu.SemaphoreType.DMA
    seq = [jax.ShapeDtypeStruct((num_dev, rows, n), bf) for n in (width, width, dim)]
    own = [jax.ShapeDtypeStruct((rows, n), bf) for n in (q_width, dim)]
    return pl.pallas_call(
        functools.partial(gather_kernel, num_dev, layer, shift),
        in_specs=[any_] * 4,
        out_specs=[any_] * 5,
        out_shape=seq + own,
        scratch_shapes=[pltpu.VMEM((dim,) + s, bf) for s in shapes] + [pltpu.VMEM((dim, n), bf) for n in (q_width, width, width)]
        + [pltpu.VMEM((2, rows, dim), bf), pltpu.VMEM((rows, dim), bf)] + [pltpu.VMEM((2, rows, width), bf)] * 2 + [pltpu.VMEM((rows, q_width), bf)]
        + [sem((3,)), sem((2,)), sem((2, 2))] + [sem((2, hops + 1, 2))] * 4,
        compiler_params=params(collective_id=1, has_side_effects=True),
        cost_estimate=pl.CostEstimate(flops=4 * rows * num_dev * dim * width, bytes_accessed=4 * dim * width, transcendentals=0),
        name="gather",
    )(x, w_query, w_key, w_value)


def causal_kernel(layer, seq, blk_ref, q_ref, k_ref, v_ref, x_ref, w_hbm, out_ref, o_s, w_s, upd_s, acc_s, top_s, tot_s, sem):
    g = pl.program_id(0)
    wcopy = pltpu.make_async_copy(w_hbm.at[layer], w_s, sem)

    @pl.when(g == 0)
    def _():
        wcopy.start()

    lead, trail = blk_ref[0], blk_ref[1]
    tile = 4 * BLK
    lanes = tot_s.shape[-1]
    per = tile // BLK
    front = seq // 2 // tile
    num_trail = lax.div(trail + 1 + per - 1, per) - front
    factor = LOG2_E * BLK ** -0.5
    def scores(item):
        _, qrow, t, limit, h = item
        q = q_ref[pl.ds(qrow, BLK), h * BLK:(h + 1) * BLK]
        s = lax.dot_general(q, k_ref[pl.ds(t, tile), :], (((1,), (1,)), ((), ())), preferred_element_type=jnp.float32)
        if limit is not None:
            reach = lax.broadcasted_iota(jnp.int32, (BLK, 1), 0) + limit
            s = jnp.where(lax.broadcasted_iota(jnp.int32, s.shape, 1) <= reach, s, NEG_BIG)
        return s

    def finish(s, item):
        slot, _, t, _, h = item
        top = jnp.max(s, axis=-1, keepdims=True)
        e = jnp.exp2((s - top) * factor)
        tot_s[slot, h] = functools.reduce(jnp.add, [e[:, i * lanes:(i + 1) * lanes] for i in range(tile // lanes)])
        acc_s[slot, h] = jnp.dot(e.astype(jnp.bfloat16), v_ref[pl.ds(t, tile), :], preferred_element_type=jnp.float32)
        top_s[slot, h] = top

    items = []
    for j in range(front + 1):
        late = j < num_trail
        t = jnp.where(late, front + j, j - num_trail) * tile
        second = (front + j, pl.multiple_of(jnp.where(late, BLK, 0), BLK), pl.multiple_of(t, tile), jnp.where(late, trail, lead) * BLK - t)
        for chain in ([(j, BLK, j * tile, None)] if j < front else []) + [second]:
            items += [chain + (h,) for h in range(2)]
    ready = scores(items[0])
    for i, item in enumerate(items):
        now = ready
        if i + 1 < len(items):
            ready = scores(items[i + 1])
        finish(now, item)

    for h in range(2):
        cols = pl.ds(pl.multiple_of(g * 2 * BLK + h * BLK, BLK), BLK)
        for i, slots in enumerate((range(front, 2 * front + 1), range(2 * front + 1))):
            tops = []
            for slot in slots:
                late = slot < front + num_trail
                tops.append(jnp.where(late if i == 1 else jnp.logical_not(late), top_s[slot, h], NEG_BIG))
            new = functools.reduce(jnp.maximum, tops)
            acc = total = None
            for slot, top in zip(slots, tops):
                fix = jnp.exp2((top - new) * factor)
                a, b = acc_s[slot, h] * fix, tot_s[slot, h] * fix
                acc, total = (a, b) if acc is None else (acc + a, total + b)
            o_s[i * BLK:(i + 1) * BLK, cols] = (acc / jnp.sum(total, axis=-1, keepdims=True)).astype(jnp.bfloat16)

    @pl.when(g == pl.num_programs(0) - 1)
    def _():
        wcopy.wait()
        output_rows(o_s, w_s, x_ref, out_ref, upd_s)


def causal_layer(blocks, q, k_all, v_all, x, w_out, layer):
    rows, dim = x.shape
    seq = k_all.shape[0]
    slots = 2 * (seq // 2 // (4 * BLK)) + 1
    kv = pl.BlockSpec((seq, BLK), lambda g, b: (0, g))
    row = pl.BlockSpec((rows, dim), lambda g, b: (0, 0))
    return pl.pallas_call(
        functools.partial(causal_kernel, layer, seq),
        grid_spec=pltpu.PrefetchScalarGridSpec(
            num_scalar_prefetch=1,
            grid=(k_all.shape[1] // BLK,),
            in_specs=[pl.BlockSpec((rows, 2 * BLK), lambda g, b: (0, g)), kv, kv, row, pl.BlockSpec(memory_space=pl.ANY)],
            out_specs=row,
            scratch_shapes=[
                pltpu.VMEM(q.shape, jnp.bfloat16),
                pltpu.VMEM(w_out.shape[1:], jnp.bfloat16),
                pltpu.VMEM((rows, dim), jnp.float32),
                pltpu.VMEM((slots, 2, BLK, BLK), jnp.float32),
                pltpu.VMEM((slots, 2, BLK, 1), jnp.float32),
                pltpu.VMEM((slots, 2, BLK, 128), jnp.float32),
                pltpu.SemaphoreType.DMA,
            ],
        ),
        out_shape=jax.ShapeDtypeStruct((rows, dim), jnp.bfloat16),
        compiler_params=params(),
        cost_estimate=pl.CostEstimate(flops=30 * 10 ** 9, bytes_accessed=2 * w_out[0].size, transcendentals=0),
        name="causal",
    )(blocks, q, k_all, v_all, x, w_out)


def solution(mesh):
    num_dev = mesh.shape["cp"]

    def per_device(hidden, w_query, w_key, w_value, w_out):
        rank = lax.axis_index("cp")
        num_layers = w_query.shape[0]
        rows, dim = hidden.shape
        w_out = w_out.reshape(num_layers, -1, dim)
        last = num_layers - 1
        x = window_stack(hidden, w_query, w_key, w_value, w_out, last, num_dev)
        k_all, v_all, _, q, x_fin = gather_keys(x, w_query, w_key, w_value, last, last, num_dev)
        blocks = jnp.stack([rank, 2 * num_dev - 1 - rank]).astype(jnp.int32)
        return causal_layer(blocks, q, k_all.reshape(-1, k_all.shape[-1]), v_all.reshape(-1, v_all.shape[-1]), x_fin, w_out, last)

    row_spec = P(("dp", "cp"), None)
    return jax.shard_map(per_device, mesh=mesh, in_specs=(row_spec, P(), P(), P(), P()), out_specs=row_spec, check_vma=False)
```

```python
import functools

import jax
import jax.numpy as jnp
from jax import lax
from jax.experimental import pallas as pl
from jax.experimental.pallas import tpu as pltpu
from jax.sharding import PartitionSpec as P

WINDOW = 1024
EPS_NORM = 1e-6
NEG_BIG = -1e30
LOG2_E = 1.4426950408889634
BLK = 256
VMEM_BYTES = 62 << 20
MESH = pl.DeviceIdType.MESH


def params(**kw):
    return pltpu.CompilerParams(vmem_limit_bytes=VMEM_BYTES, **kw)


def normed(rows):
    wide = rows.astype(jnp.float32)
    return (wide * lax.rsqrt(jnp.mean(wide * wide, axis=-1, keepdims=True) + EPS_NORM)).astype(jnp.bfloat16)


def output_rows(o_s, w_s, x_ref, out_ref, upd_s):
    rows, dim = x_ref.shape
    tile = 768

    @pl.loop(0, dim // tile)
    def _(s):
        cols = pl.ds(pl.multiple_of(s * tile, tile), tile)
        upd_s[:, cols] = jnp.dot(o_s[...], w_s[:, cols], preferred_element_type=jnp.float32)

    @pl.loop(0, rows // 64)
    def _(s):
        part = pl.ds(pl.multiple_of(s * 64, 64), 64)
        upd = upd_s[part, :]
        scale = lax.rsqrt(jnp.mean(upd * upd, axis=-1, keepdims=True) + EPS_NORM)
        out_ref[part, :] = (x_ref[part, :].astype(jnp.float32) + upd * scale).astype(jnp.bfloat16)


def scoped(name):
    def wrap(fn):
        def run(*args):
            with jax.named_scope(name):
                return fn(*args)

        return run

    return wrap


def stack_kernel(num_dev, num_layers, x_hbm, wq_hbm, wk_hbm, wv_hbm, wo_hbm, x_all,
                 xr, xn, kv, n_s, q_s, wq_s, wkv_s, wo_s, upd_s, stq, stk, stv,
                 g_send, g_recv, x_send, x_recv, h_send, h_recv, c_send, c_recv, h_free, c_free, xsem, qsem, ksem, vsem, wsem):
    blk, dim = n_s.shape
    width = wkv_s.shape[1] // 2
    heads = q_s.shape[2] // width
    head = BLK
    q_rows, kv_rows = stq.shape[1], stk.shape[1]
    q_ring, kv_ring = stq.shape[0], stk.shape[0]
    q_parts, kv_parts = dim // q_rows, dim // kv_rows
    me = lax.axis_index("cp")
    odd = lax.rem(me, 2)
    is_odd, is_even = odd == 1, odd == 0
    left, right = lax.rem(me + num_dev - 1, num_dev), lax.rem(me + 1, num_dev)

    other = jnp.where(is_odd, left, right)
    peers = (lax.rem(me + 2, num_dev), lax.rem(me + num_dev - 2, num_dev), other)
    sources = (peers[1], peers[0], other)

    def block(i):
        return pl.ds(pl.multiple_of(i * blk, blk), blk)

    def remote(src, dst, send, recv, dev):
        return pltpu.make_async_remote_copy(src_ref=src, dst_ref=dst, send_sem=send, recv_sem=recv, device_id={"cp": dev}, device_id_type=MESH)

    def x_copy(slot, s):
        return remote(xn.at[s], xr.at[slot, s], x_send.at[s], x_recv.at[slot, s], left)

    def g_copy(i, owner):
        return remote(xn.at[0], x_all.at[owner, block(0)], g_send.at[i], g_recv.at[i], peers[i])

    def keep(s):
        return pltpu.make_async_copy(xn.at[s], x_all.at[me, block(s)], xsem.at[s])

    def h_copy(s):
        return remote(kv.at[block(2 + s)], kv.at[block(s)], h_send.at[s], h_recv.at[s], right)

    def c_copy(s):
        return remote(kv.at[block(2 + s)], kv.at[block(4 + s)], c_send.at[s], c_recv.at[s], left)

    def signal(sem, dev):
        pl.semaphore_signal(sem, inc=1, device_id={"cp": dev}, device_id_type=MESH)

    def q_stage(layer, i):
        b = lax.rem(layer * q_parts + i, q_ring)
        return pltpu.make_async_copy(wq_hbm.at[layer, pl.ds(i * q_rows, q_rows)], stq.at[b], qsem.at[b])

    def kv_stage(layer, i):
        b = lax.rem(layer * kv_parts + i, kv_ring)
        rows = pl.ds(i * kv_rows, kv_rows)
        return (pltpu.make_async_copy(wk_hbm.at[layer, rows], stk.at[b], ksem.at[b]),
                pltpu.make_async_copy(wv_hbm.at[layer, rows], stv.at[b], vsem.at[b]))

    def kv_start(layer, i):
        for cp in kv_stage(layer, i):
            cp.start()

    def kv_wait(layer, i):
        for cp in kv_stage(layer, i):
            cp.wait()

    def kv_flat(layer, i):
        b = lax.rem(layer * kv_parts + i, kv_ring)
        rows = pl.ds(pl.multiple_of(i * kv_rows, 16), kv_rows)
        wkv_s[rows, :width] = stk[b].reshape(kv_rows, width)
        wkv_s[rows, width:] = stv[b].reshape(kv_rows, width)

    def q_flat(layer, i):
        b = lax.rem(layer * q_parts + i, q_ring)
        wq_s[pl.ds(pl.multiple_of(i * q_rows, 16), q_rows), :] = stq[b].reshape(q_rows, wq_s.shape[1])

    def kv_next(layer, i):
        @pl.when(i + kv_ring < kv_parts)
        def _():
            kv_start(layer, i + kv_ring)

    def q_next(layer, i):
        after = i + q_ring

        @pl.when(after < q_parts)
        def _():
            q_stage(layer, after).start()

        @pl.when((after >= q_parts) & (layer + 1 < num_layers))
        def _():
            q_stage(layer + 1, after - q_parts).start()

    def wo_copy(layer):
        return pltpu.make_async_copy(wo_hbm.at[layer], wo_s, wsem)

    def norm_into(ref):
        step = min(64, blk)

        @pl.loop(0, blk // step)
        def _(i):
            part = pl.ds(pl.multiple_of(i * step, step), step)
            n_s[part, :] = normed(ref[part, :])

    def dot(w):
        return jnp.dot(n_s[...], w, preferred_element_type=jnp.float32).astype(jnp.bfloat16)

    def attend(s, span, start):
        window = WINDOW + blk
        rows = pl.ds(pl.multiple_of(s * blk + window - span, blk), span)
        factor = LOG2_E * head ** -0.5
        groups = width // head
        together = groups if span == window else 2
        qi = lax.broadcasted_iota(jnp.int32, (blk, blk), 0)
        ki = lax.broadcasted_iota(jnp.int32, (blk, blk), 1)

        def scores(item):
            sc = lax.dot_general(q_s[s, :, item[2]], kv[rows, item[0]], (((1,), (1,)), ((), ())), preferred_element_type=jnp.float32)
            last = jnp.where(ki <= qi, sc[:, span - blk:], NEG_BIG)
            if span == window:
                return jnp.concatenate([jnp.where(ki > qi, sc[:, :blk], NEG_BIG), sc[:, blk:span - blk], last], axis=1)
            mid = sc[:, :span - blk]
            pos = lax.broadcasted_iota(jnp.int32, mid.shape, 1)
            return jnp.concatenate([jnp.where(pos >= start - (window - span), mid, NEG_BIG), last], axis=1)

        def finish(sc, item):
            top = jnp.max(sc, axis=-1, keepdims=True)
            e = jnp.exp2((sc - top) * factor)
            total = jnp.sum(e, axis=-1, keepdims=True)
            acc = jnp.dot(e.astype(jnp.bfloat16), kv[rows, item[1]], preferred_element_type=jnp.float32)
            return (acc / total).astype(jnp.bfloat16)

        def some(first):
            items = []
            for u in range(together):
                g = first + u
                for h in range(heads):
                    offsets = (g * head, width + g * head, (g * heads + h) * head)
                    items.append(tuple(pl.ds(o if isinstance(o, int) else pl.multiple_of(o, head), head) for o in offsets))
            ahead = scores(items[0])
            for k, item in enumerate(items):
                now = ahead
                if k + 1 < len(items):
                    ahead = scores(items[k + 1])
                q_s[s, :, item[2]] = finish(now, item)

        if together == groups:
            some(0)
        else:
            @pl.loop(0, groups // together)
            def _(i):
                some(i * together)

    tile = width
    loads = [pltpu.make_async_copy(x_hbm.at[block(s)], xn.at[s], xsem.at[s]) for s in range(2)]
    for cp in loads:
        cp.start()
    for i in range(kv_ring):
        kv_start(0, i)
    for i in range(q_ring):
        q_stage(0, i).start()
    barrier = pltpu.get_barrier_semaphore()
    for dev in (left, right) + peers[:2]:
        signal(barrier, dev)
    pl.semaphore_wait(barrier, 4)
    for s in range(2):
        loads[s].wait()
        x_copy(0, s).start()

    @pl.loop(0, kv_parts)
    def _(i):
        kv_wait(0, i)
        kv_flat(0, i)
        kv_next(0, i)

    @pl.loop(0, num_layers)
    def _(layer):
        slot = lax.rem(layer, 2)
        more = layer + 1 < num_layers
        chunk = lax.rem(me + layer + 1, num_dev)

        @pl.when(layer > 0)
        def _():
            for s in range(2):
                h_copy(s).wait_send()

            @pl.when(is_odd)
            def _():
                for s in range(2):
                    c_copy(s).wait_send()

        @pl.loop(0, 2)
        def _(s):
            with jax.named_scope("own_norm"):
                norm_into(xn.at[s])

            @pl.loop(0, 2)
            @scoped("own")
            def _(j):
                cols = pl.ds(pl.multiple_of(j * tile, tile), tile)
                kv[block(2 + s), cols] = dot(wkv_s[:, cols])

            @pl.when((layer > 0) & (s == 0))
            @scoped("credit")
            def _():
                pl.semaphore_wait(h_free, 1)

                @pl.when(is_odd)
                def _():
                    pl.semaphore_wait(c_free, 1)

            h_copy(s).start()

            @pl.when(is_odd)
            def _():
                c_copy(s).start()

        @pl.loop(0, q_parts)
        @scoped("q_lay")
        def _(i):
            q_stage(layer, i).wait()
            q_flat(layer, i)
            q_next(layer, i)

        wo_copy(layer).start()

        @pl.when(more)
        def _():
            for i in range(kv_ring):
                kv_start(layer + 1, i)

        @pl.loop(0, 2)
        def _(s):
            @pl.loop(jnp.where(is_odd, s, 2 * s), jnp.where(is_odd, s + 1, 2))
            def _(t):
                with jax.named_scope("x_wait"):
                    x_copy(slot, t).wait_recv()
                with jax.named_scope("norm"):
                    norm_into(xr.at[slot, t])

                @pl.loop(0, 2)
                @scoped("query")
                def _(j):
                    cols = pl.ds(pl.multiple_of(j * tile, tile), tile)
                    q_s[t, :, cols] = dot(wq_s[:, cols])

                @pl.when(is_odd)
                def _():
                    @pl.loop(0, 2)
                    @scoped("keys")
                    def _(j):
                        cols = pl.ds(pl.multiple_of(j * tile, tile), tile)
                        kv[block(4 + t), cols] = dot(wkv_s[:, cols])

            @pl.when(s == 0)
            @scoped("h_wait")
            def _():
                for i in range(2):
                    h_copy(i).wait_recv()

            @pl.when(is_even)
            @scoped("c_wait")
            def _():
                c_copy(s).wait_recv()

            for first, cond in ((2, chunk >= 2), (1, chunk == 1), (0, chunk == 0)):
                @pl.when(cond)
                @scoped("attend")
                def _():
                    attend(s, (2 * first + 1) * blk if first == 2 else (2 * first + 2) * blk, WINDOW - s * blk - first * 2 * blk)

            @pl.when((s == 1) & more)
            def _():
                signal(h_free, left)

                @pl.when(is_even)
                def _():
                    signal(c_free, right)

            out_tiles = 3
            out_tile = dim // out_tiles

            @pl.when(s == 0)
            def _():
                wo_copy(layer).wait()

            def out_dot(j):
                cols = pl.ds(pl.multiple_of(j * out_tile, out_tile), out_tile)
                upd_s[:, cols] = jnp.dot(q_s[s], wo_s[:, cols], preferred_element_type=jnp.float32)

            relay = (s == 1) & more

            @pl.when(relay)
            def _():
                @pl.loop(0, out_tiles)
                @scoped("out_lay")
                def _(j):
                    per = kv_parts // out_tiles
                    for t in range(per):
                        kv_wait(layer + 1, j * per + t)
                        kv_flat(layer + 1, j * per + t)
                        kv_next(layer + 1, j * per + t)
                    out_dot(j)

            @pl.when(jnp.logical_not(relay))
            def _():
                @pl.loop(0, out_tiles)
                @scoped("out")
                def _(j):
                    out_dot(j)

            with jax.named_scope("x_sent"):
                x_copy(slot, s).wait_send()
            step = min(64, blk)

            @pl.loop(0, blk // step)
            @scoped("resid")
            def _(i):
                part = pl.ds(pl.multiple_of(i * step, step), step)
                upd = upd_s[part, :]
                scale = lax.rsqrt(jnp.mean(upd * upd, axis=-1, keepdims=True) + EPS_NORM)
                xn[s, part, :] = (xr[slot, s, part, :].astype(jnp.float32) + upd * scale).astype(jnp.bfloat16)

            @pl.when(more)
            def _():
                x_copy(1 - slot, s).start()

            @pl.when(jnp.logical_not(more))
            def _():
                keep(s).start()

                @pl.when(s == 0)
                def _():
                    for i in range(3):
                        g_copy(i, me).start()

    for s in range(2):
        h_copy(s).wait_send()
        keep(s).wait()

    @pl.when(is_odd)
    def _():
        for s in range(2):
            c_copy(s).wait_send()

    for i in range(3):
        g_copy(i, me).wait_send()
        g_copy(i, sources[i]).wait_recv()


def window_stack(x, w_query, w_key, w_value, w_out, num_layers, num_dev):
    rows, dim = x.shape
    blk = rows // 2
    q_heads, head = w_query.shape[2:]
    kv_heads = w_key.shape[2]
    q_width, width = q_heads * head, kv_heads * head
    q_rows, q_ring, kv_rows, kv_ring = dim // 8, 4, dim // 9, 4
    any_ = pl.BlockSpec(memory_space=pl.ANY)
    bf = jnp.bfloat16
    dma, regular = pltpu.SemaphoreType.DMA, pltpu.SemaphoreType.REGULAR
    return pl.pallas_call(
        functools.partial(stack_kernel, num_dev, num_layers),
        in_specs=[any_] * 5,
        out_specs=any_,
        out_shape=jax.ShapeDtypeStruct((num_dev, rows, dim), bf),
        scratch_shapes=[
            pltpu.VMEM((2, 2, blk, dim), bf),
            pltpu.VMEM((2, blk, dim), bf),
            pltpu.VMEM((6 * blk, 2 * width), bf),
            pltpu.VMEM((blk, dim), bf),
            pltpu.VMEM((2, blk, q_width), bf),
            pltpu.VMEM((dim, q_width), bf),
            pltpu.VMEM((dim, 2 * width), bf),
            pltpu.VMEM((q_width, dim), bf),
            pltpu.VMEM((blk, dim), jnp.float32),
            pltpu.VMEM((q_ring, q_rows, q_heads, head), bf),
            pltpu.VMEM((kv_ring, kv_rows, kv_heads, head), bf),
            pltpu.VMEM((kv_ring, kv_rows, kv_heads, head), bf),
            dma((3,)), dma((3,)), dma((2,)), dma((2, 2)), dma((2,)), dma((2,)), dma((2,)), dma((2,)),
            regular, regular, dma((2,)), dma((q_ring,)), dma((kv_ring,)), dma((kv_ring,)), dma,
        ],
        compiler_params=pltpu.CompilerParams(vmem_limit_bytes=67043328, collective_id=2, has_side_effects=True),
        cost_estimate=pl.CostEstimate(flops=num_layers * 20 * 10 ** 9, bytes_accessed=num_layers * 28 * 10 ** 6, transcendentals=0),
        name="stack",
    )(x, w_query, w_key, w_value, w_out)


def norm_rows(src, dst):
    rows = src.shape[0]
    step = min(64, rows)

    @pl.loop(0, rows // step)
    def _(i):
        part = pl.ds(pl.multiple_of(i * step, step), step)
        dst[part, :] = normed(src[part, :])


def gather_kernel(num_dev, layer, shift, x_in, wq_hbm, wk_hbm, wv_hbm, k_all, v_all, x_all, q_hbm, x_fin,
                  wq_st, wk_st, wv_st, wq_s, wk_s, wv_s, x_s, n_s, k_s, v_s, q_s, f_s, wsem, fsem, lsem, ssem, send, recv, psend, precv):
    _, rows, dim = x_s.shape
    half = rows // 2
    me = lax.axis_index("cp")
    other = me + 1 - 2 * lax.rem(me, 2)
    near = (lax.rem(me + 2, num_dev), lax.rem(me + num_dev - 2, num_dev))
    hops = num_dev // 4

    def wrap(v):
        return lax.rem(v + 4 * num_dev, num_dev)

    def owner(dev, way, hop):
        if isinstance(way, int):
            return wrap(dev - 2 * hop) if way == 0 else wrap(dev + 2 * hop)
        return wrap(dev + jnp.where(way == 0, -2, 2) * hop)

    def piece(dev, h):
        return x_all.at[dev, pl.ds(h * half, half)]

    def link(way, hop, h):
        ref = piece(owner(me, way, hop - 1), h)
        return pltpu.make_async_remote_copy(src_ref=ref, dst_ref=ref, send_sem=send.at[way, hop, h], recv_sem=recv.at[way, hop, h],
                                            device_id={"cp": near[way]}, device_id_type=MESH)

    def landed(way, hop, h):
        ref = piece(owner(me, way, hop), h)
        return pltpu.make_async_remote_copy(src_ref=ref, dst_ref=ref, send_sem=send.at[way, hop, h], recv_sem=recv.at[way, hop, h],
                                            device_id={"cp": near[way]}, device_id_type=MESH)

    def across(way, hop, h, dev):
        ref = piece(owner(dev, way, hop), h)
        return pltpu.make_async_remote_copy(src_ref=ref, dst_ref=ref, send_sem=psend.at[way, hop, h], recv_sem=precv.at[way, hop, h],
                                            device_id={"cp": other}, device_id_type=MESH)

    def finals():
        copies = []
        for i, block in enumerate((me, 2 * num_dev - 1 - me)):
            src = wrap(lax.div(block, 2) - shift)
            copies.append(pltpu.make_async_copy(piece(src, lax.rem(block, 2)), f_s.at[pl.ds(i * half, half)], fsem.at[i]))
        return copies

    wcopies = [pltpu.make_async_copy(w.at[layer], st, wsem.at[i]) for i, (w, st) in enumerate(((wk_hbm, wk_st), (wv_hbm, wv_st), (wq_hbm, wq_st)))]
    for cp in wcopies:
        cp.start()
    barrier = pltpu.get_barrier_semaphore()
    for dev in near + (other,):
        pl.semaphore_signal(barrier, inc=1, device_id={"cp": dev}, device_id_type=MESH)
    pl.semaphore_wait(barrier, 3)
    for way in range(2):
        link(way, 1, 1).start()
    across(0, 0, 1, me).start()
    for way in range(2):
        link(way, 2, 0).start()
        across(way, 1, 0, me).start()
    for cp in wcopies:
        cp.wait()
    step_rows = 256

    @pl.loop(0, dim // step_rows)
    def _(s):
        part = pl.ds(pl.multiple_of(s * step_rows, step_rows), step_rows)
        wk_s[part, :] = wk_st[part].reshape(step_rows, -1)
        wv_s[part, :] = wv_st[part].reshape(step_rows, -1)
        wq_s[part, :] = wq_st[part].reshape(step_rows, -1)

    @pl.loop(0, hops + 1)
    def _(hop):
        for h in range(2):
            for way in range(2):
                last_ok = way == h

                def arrive():
                    with jax.named_scope("land"):
                        landed(way, hop, h).wait_recv()
                    if last_ok:
                        @pl.when(hop < hops)
                        def _():
                            link(way, hop + 1, h).start()
                    else:
                        @pl.when(hop < hops - 1)
                        def _():
                            link(way, hop + 1, h).start()
                    across(way, hop, h, me).start()

                first_hop = 2 - h
                if last_ok:
                    pl.when(hop >= first_hop)(arrive)
                else:
                    pl.when((hop >= first_hop) & (hop < hops))(arrive)

        whole = (hop > 0) & (hop < hops)
        count = jnp.where(whole, 4, 2)

        def source(a):
            mine = a < lax.div(count, 2)
            way = jnp.where(whole, lax.rem(a, 2), 0)
            return mine, way, wrap(jnp.where(mine, me, other) + jnp.where(way == 0, -2, 2) * hop)

        def load(a):
            b = lax.rem(a, 2)
            return pltpu.make_async_copy(x_all.at[source(a)[2]], x_s.at[b], lsem.at[b])

        def stores(a):
            b = lax.rem(a, 2)
            chunk = wrap(source(a)[2] + shift)
            return [pltpu.make_async_copy(t.at[b], o.at[chunk], ssem.at[i, b]) for i, (t, o) in enumerate(((k_s, k_all), (v_s, v_all)))]

        def fetch(a):
            mine, way, _ = source(a)

            @pl.when(jnp.logical_not(mine))
            @scoped("cross")
            def _():
                @pl.when(hop > 0)
                def _():
                    across(jnp.where(hop == hops, 0, way), hop, 0, other).wait_recv()

                across(jnp.where(hop == hops, 1, way), hop, 1, other).wait_recv()

            load(a).start()

        fetch(0)

        @pl.loop(0, count)
        def _(a):
            b = lax.rem(a, 2)

            with jax.named_scope("load"):
                load(a).wait()
            with jax.named_scope("norm"):
                norm_rows(x_s.at[b], n_s)

            @pl.when(a + 1 < count)
            def _():
                fetch(a + 1)

            @pl.when((hop == hops) & (a == 0))
            def _():
                for cp in finals():
                    cp.start()

            @pl.when(a >= 2)
            @scoped("store")
            def _():
                for cp in stores(a - 2):
                    cp.wait()

            with jax.named_scope("keys"):
                k_s[b] = jnp.dot(n_s[...], wk_s[...], preferred_element_type=jnp.float32).astype(jnp.bfloat16)
                v_s[b] = jnp.dot(n_s[...], wv_s[...], preferred_element_type=jnp.float32).astype(jnp.bfloat16)
            for cp in stores(a):
                cp.start()

        for back in range(2):
            for cp in stores(count - 2 + back):
                cp.wait()

    for cp in finals():
        cp.wait()
    keep = pltpu.make_async_copy(f_s, x_fin, lsem.at[0])
    keep.start()
    norm_rows(f_s, n_s)
    with jax.named_scope("query"):
        q_s[...] = jnp.dot(n_s[...], wq_s[...], preferred_element_type=jnp.float32).astype(jnp.bfloat16)
    last = pltpu.make_async_copy(q_s, q_hbm, lsem.at[1])
    last.start()
    last.wait()
    keep.wait()
    for way in range(2):
        for hop in range(1, hops + 1):
            for h in range(2):
                if hop < hops or way == h:
                    across(way, hop, h, me).wait_send()
                    if hop + h > 1:
                        link(way, hop, h).wait_send()
    across(0, 0, 1, me).wait_send()


def gather_keys(x_all, w_query, w_key, w_value, layer, shift, num_dev):
    _, rows, dim = x_all.shape
    shapes = [w.shape[2:] for w in (w_query, w_key, w_value)]
    q_width, width = (h * e for h, e in shapes[:2])
    hops = num_dev // 4
    any_ = pl.BlockSpec(memory_space=pl.ANY)
    bf = jnp.bfloat16
    sem = pltpu.SemaphoreType.DMA
    seq = [jax.ShapeDtypeStruct((num_dev, rows, n), bf) for n in (width, width, dim)]
    own = [jax.ShapeDtypeStruct((rows, n), bf) for n in (q_width, dim)]
    return pl.pallas_call(
        functools.partial(gather_kernel, num_dev, layer, shift),
        in_specs=[any_] * 4,
        out_specs=[any_] * 5,
        out_shape=seq + own,
        input_output_aliases={0: 2},
        scratch_shapes=[pltpu.VMEM((dim,) + s, bf) for s in shapes] + [pltpu.VMEM((dim, n), bf) for n in (q_width, width, width)]
        + [pltpu.VMEM((2, rows, dim), bf), pltpu.VMEM((rows, dim), bf)] + [pltpu.VMEM((2, rows, width), bf)] * 2 + [pltpu.VMEM((rows, q_width), bf), pltpu.VMEM((rows, dim), bf)]
        + [sem((3,)), sem((2,)), sem((2,)), sem((2, 2))] + [sem((2, hops + 1, 2))] * 4,
        compiler_params=params(collective_id=1, has_side_effects=True),
        cost_estimate=pl.CostEstimate(flops=4 * rows * num_dev * dim * width, bytes_accessed=4 * dim * width, transcendentals=0),
        name="gather",
    )(x_all, w_query, w_key, w_value)


def causal_kernel(layer, seq, blk_ref, q_ref, k_ref, v_ref, x_ref, w_hbm, out_ref, o_s, w_s, upd_s, acc_s, top_s, tot_s, sem):
    g = pl.program_id(0)
    wcopy = pltpu.make_async_copy(w_hbm.at[layer], w_s, sem)

    @pl.when(g == 0)
    def _():
        wcopy.start()

    lead, trail = blk_ref[0], blk_ref[1]
    tile = 4 * BLK
    lanes = tot_s.shape[-1]
    per = tile // BLK
    front = seq // 2 // tile
    num_trail = lax.div(trail + 1 + per - 1, per) - front
    factor = LOG2_E * BLK ** -0.5
    def scores(item):
        _, qrow, t, limit, h = item
        q = q_ref[pl.ds(qrow, BLK), h * BLK:(h + 1) * BLK]
        s = lax.dot_general(q, k_ref[pl.ds(t, tile), :], (((1,), (1,)), ((), ())), preferred_element_type=jnp.float32)
        if limit is not None:
            reach = lax.broadcasted_iota(jnp.int32, (BLK, 1), 0) + limit
            s = jnp.where(lax.broadcasted_iota(jnp.int32, s.shape, 1) <= reach, s, NEG_BIG)
        return s

    def finish(s, item):
        slot, _, t, _, h = item
        top = jnp.max(s, axis=-1, keepdims=True)
        e = jnp.exp2((s - top) * factor)
        tot_s[slot, h] = functools.reduce(jnp.add, [e[:, i * lanes:(i + 1) * lanes] for i in range(tile // lanes)])
        acc_s[slot, h] = jnp.dot(e.astype(jnp.bfloat16), v_ref[pl.ds(t, tile), :], preferred_element_type=jnp.float32)
        top_s[slot, h] = top

    items = []
    for j in range(front):
        chains = [(j, BLK, j * tile, None)]
        if j < 2:
            block, t = ((trail, front + num_trail - 1), (lead, front - num_trail))[j]
            t = pl.multiple_of(t * tile, tile)
            chains.append((front + j, (1 - j) * BLK, t, block * BLK - t))
        if j > 0:
            late = j < num_trail
            t = jnp.where(late, front + j - 1, j - num_trail) * tile
            chains.append((front + 1 + j, pl.multiple_of(jnp.where(late, BLK, 0), BLK), pl.multiple_of(t, tile), None))
        for chain in chains:
            items += [chain + (h,) for h in range(2)]
    ready = scores(items[0])
    for i, item in enumerate(items):
        now = ready
        if i + 1 < len(items):
            ready = scores(items[i + 1])
        finish(now, item)

    for h in range(2):
        cols = pl.ds(pl.multiple_of(g * 2 * BLK + h * BLK, BLK), BLK)
        shared = range(front + 2, 2 * front + 1)
        for i, slots in enumerate(([front + 1, *shared], [*range(front + 1), *shared])):
            tops = []
            for slot in slots:
                top = top_s[slot, h]
                if slot > front + 1:
                    late = slot - front - 1 < num_trail
                    top = jnp.where(late if i == 1 else jnp.logical_not(late), top, NEG_BIG)
                tops.append(top)
            new = functools.reduce(jnp.maximum, tops)
            acc = total = None
            for slot, top in zip(slots, tops):
                fix = jnp.exp2((top - new) * factor)
                a, b = acc_s[slot, h] * fix, tot_s[slot, h] * fix
                acc, total = (a, b) if acc is None else (acc + a, total + b)
            o_s[i * BLK:(i + 1) * BLK, cols] = (acc / jnp.sum(total, axis=-1, keepdims=True)).astype(jnp.bfloat16)

    @pl.when(g == pl.num_programs(0) - 1)
    def _():
        wcopy.wait()
        output_rows(o_s, w_s, x_ref, out_ref, upd_s)


def causal_layer(blocks, q, k_all, v_all, x, w_out, layer):
    rows, dim = x.shape
    seq = k_all.shape[0]
    slots = 2 * (seq // 2 // (4 * BLK)) + 1
    kv = pl.BlockSpec((seq, BLK), lambda g, b: (0, g))
    row = pl.BlockSpec((rows, dim), lambda g, b: (0, 0))
    return pl.pallas_call(
        functools.partial(causal_kernel, layer, seq),
        grid_spec=pltpu.PrefetchScalarGridSpec(
            num_scalar_prefetch=1,
            grid=(k_all.shape[1] // BLK,),
            in_specs=[pl.BlockSpec((rows, 2 * BLK), lambda g, b: (0, g)), kv, kv, row, pl.BlockSpec(memory_space=pl.ANY)],
            out_specs=row,
            scratch_shapes=[
                pltpu.VMEM(q.shape, jnp.bfloat16),
                pltpu.VMEM(w_out.shape[1:], jnp.bfloat16),
                pltpu.VMEM((rows, dim), jnp.float32),
                pltpu.VMEM((slots, 2, BLK, BLK), jnp.float32),
                pltpu.VMEM((slots, 2, BLK, 1), jnp.float32),
                pltpu.VMEM((slots, 2, BLK, 128), jnp.float32),
                pltpu.SemaphoreType.DMA,
            ],
        ),
        out_shape=jax.ShapeDtypeStruct((rows, dim), jnp.bfloat16),
        compiler_params=params(),
        cost_estimate=pl.CostEstimate(flops=30 * 10 ** 9, bytes_accessed=2 * w_out[0].size, transcendentals=0),
        name="causal",
    )(blocks, q, k_all, v_all, x, w_out)


def solution(mesh):
    num_dev = mesh.shape["cp"]

    def per_device(hidden, w_query, w_key, w_value, w_out):
        rank = lax.axis_index("cp")
        num_layers = w_query.shape[0]
        rows, dim = hidden.shape
        w_out = w_out.reshape(num_layers, -1, dim)
        last = num_layers - 1
        x = window_stack(hidden, w_query, w_key, w_value, w_out, last, num_dev)
        k_all, v_all, _, q, x_fin = gather_keys(x, w_query, w_key, w_value, last, last, num_dev)
        blocks = jnp.stack([rank, 2 * num_dev - 1 - rank]).astype(jnp.int32)
        return causal_layer(blocks, q, k_all.reshape(-1, k_all.shape[-1]), v_all.reshape(-1, v_all.shape[-1]), x_fin, w_out, last)

    row_spec = P(("dp", "cp"), None)
    return jax.shard_map(per_device, mesh=mesh, in_specs=(row_spec, P(), P(), P(), P()), out_specs=row_spec, check_vma=False)
```

```python
import functools

import jax
import jax.numpy as jnp
from jax import lax
from jax.experimental import pallas as pl
from jax.experimental.pallas import tpu as pltpu
from jax.sharding import PartitionSpec as P

WINDOW = 1024
EPS_NORM = 1e-6
NEG_BIG = -1e30
LOG2_E = 1.4426950408889634
BLK = 256
VMEM_BYTES = 62 << 20
MESH = pl.DeviceIdType.MESH


def params(**kw):
    return pltpu.CompilerParams(vmem_limit_bytes=VMEM_BYTES, **kw)


def normed(rows):
    wide = rows.astype(jnp.float32)
    return (wide * lax.rsqrt(jnp.mean(wide * wide, axis=-1, keepdims=True) + EPS_NORM)).astype(jnp.bfloat16)


def output_rows(o_s, w_s, x_ref, out_ref, upd_s):
    rows, dim = x_ref.shape
    tile = 768

    @pl.loop(0, dim // tile)
    def _(s):
        cols = pl.ds(pl.multiple_of(s * tile, tile), tile)
        upd_s[:, cols] = jnp.dot(o_s[...], w_s[:, cols], preferred_element_type=jnp.float32)

    @pl.loop(0, rows // 16, unroll=16)
    def _(s):
        part = pl.ds(pl.multiple_of(s * 16, 16), 16)
        upd = upd_s[part, :]
        scale = lax.rsqrt(jnp.mean(upd * upd, axis=-1, keepdims=True) + EPS_NORM)
        out_ref[part, :] = (x_ref[part, :].astype(jnp.float32) + upd * scale).astype(jnp.bfloat16)


def scoped(name):
    def wrap(fn):
        def run(*args):
            with jax.named_scope(name):
                return fn(*args)

        return run

    return wrap


def stack_kernel(num_dev, num_layers, x_hbm, wq_hbm, wk_hbm, wv_hbm, wo_hbm, x_all,
                 xr, xn, kv, n_s, q_s, wq_s, wkv_s, wo_s, upd_s, stq, stk, stv,
                 g_send, g_recv, x_send, x_recv, h_send, h_recv, c_send, c_recv, h_free, c_free, xsem, qsem, ksem, vsem, wsem):
    blk, dim = n_s.shape
    width = wkv_s.shape[1] // 2
    heads = q_s.shape[2] // width
    head = BLK
    q_rows, kv_rows = stq.shape[1], stk.shape[1]
    q_ring, kv_ring = stq.shape[0], stk.shape[0]
    q_parts, kv_parts = dim // q_rows, dim // kv_rows
    me = lax.axis_index("cp")
    odd = lax.rem(me, 2)
    is_odd, is_even = odd == 1, odd == 0
    left, right = lax.rem(me + num_dev - 1, num_dev), lax.rem(me + 1, num_dev)

    other = jnp.where(is_odd, left, right)
    peers = (lax.rem(me + 2, num_dev), lax.rem(me + num_dev - 2, num_dev), other)
    sources = (peers[1], peers[0], other)

    def block(i):
        return pl.ds(pl.multiple_of(i * blk, blk), blk)

    def remote(src, dst, send, recv, dev):
        return pltpu.make_async_remote_copy(src_ref=src, dst_ref=dst, send_sem=send, recv_sem=recv, device_id={"cp": dev}, device_id_type=MESH)

    def x_copy(slot, s):
        return remote(xn.at[s], xr.at[slot, s], x_send.at[s], x_recv.at[slot, s], left)

    def g_copy(i, owner):
        return remote(xn.at[0], x_all.at[owner, block(0)], g_send.at[i], g_recv.at[i], peers[i])

    def keep(s):
        return pltpu.make_async_copy(xn.at[s], x_all.at[me, block(s)], xsem.at[s])

    def h_copy(s, j):
        cols = pl.ds(pl.multiple_of(j * width, width), width)
        return remote(kv.at[block(2 + s), cols], kv.at[block(s), cols], h_send.at[s, j], h_recv.at[s, j], right)

    def c_copy(s):
        return remote(kv.at[block(2 + s)], kv.at[block(4 + s)], c_send.at[s], c_recv.at[s], left)

    def signal(sem, dev):
        pl.semaphore_signal(sem, inc=1, device_id={"cp": dev}, device_id_type=MESH)

    def q_stage(layer, i):
        b = lax.rem(layer * q_parts + i, q_ring)
        return pltpu.make_async_copy(wq_hbm.at[layer, pl.ds(i * q_rows, q_rows)], stq.at[b], qsem.at[b])

    def kv_stage(layer, i):
        b = lax.rem(layer * kv_parts + i, kv_ring)
        rows = pl.ds(i * kv_rows, kv_rows)
        return (pltpu.make_async_copy(wk_hbm.at[layer, rows], stk.at[b], ksem.at[b]),
                pltpu.make_async_copy(wv_hbm.at[layer, rows], stv.at[b], vsem.at[b]))

    def kv_start(layer, i):
        for cp in kv_stage(layer, i):
            cp.start()

    def kv_wait(layer, i):
        for cp in kv_stage(layer, i):
            cp.wait()

    def kv_flat(layer, i):
        b = lax.rem(layer * kv_parts + i, kv_ring)
        rows = pl.ds(pl.multiple_of(i * kv_rows, 16), kv_rows)
        wkv_s[rows, :width] = stk[b].reshape(kv_rows, width)
        wkv_s[rows, width:] = stv[b].reshape(kv_rows, width)

    def q_flat(layer, i):
        b = lax.rem(layer * q_parts + i, q_ring)
        wq_s[pl.ds(pl.multiple_of(i * q_rows, 16), q_rows), :] = stq[b].reshape(q_rows, wq_s.shape[1])

    def kv_next(layer, i):
        @pl.when(i + kv_ring < kv_parts)
        def _():
            kv_start(layer, i + kv_ring)

    def q_next(layer, i):
        after = i + q_ring

        @pl.when(after < q_parts)
        def _():
            q_stage(layer, after).start()

        @pl.when((after >= q_parts) & (layer + 1 < num_layers))
        def _():
            q_stage(layer + 1, after - q_parts).start()

    def wo_copy(layer):
        return pltpu.make_async_copy(wo_hbm.at[layer], wo_s, wsem)

    def norm_into(ref):
        step = min(16, blk)

        @pl.loop(0, blk // step, unroll=blk // step)
        def _(i):
            part = pl.ds(pl.multiple_of(i * step, step), step)
            n_s[part, :] = normed(ref[part, :])

    def dot(w):
        return jnp.dot(n_s[...], w, preferred_element_type=jnp.float32).astype(jnp.bfloat16)

    def attend(s, span, start):
        window = WINDOW + blk
        rows = pl.ds(pl.multiple_of(s * blk + window - span, blk), span)
        factor = LOG2_E * head ** -0.5
        groups = width // head
        together = groups if span == window else 2
        qi = lax.broadcasted_iota(jnp.int32, (blk, blk), 0)
        ki = lax.broadcasted_iota(jnp.int32, (blk, blk), 1)

        def scores(item):
            sc = lax.dot_general(q_s[s, :, item[2]], kv[rows, item[0]], (((1,), (1,)), ((), ())), preferred_element_type=jnp.float32)
            last = jnp.where(ki <= qi, sc[:, span - blk:], NEG_BIG)
            if span == window:
                return jnp.concatenate([jnp.where(ki > qi, sc[:, :blk], NEG_BIG), sc[:, blk:span - blk], last], axis=1)
            mid = sc[:, :span - blk]
            pos = lax.broadcasted_iota(jnp.int32, mid.shape, 1)
            return jnp.concatenate([jnp.where(pos >= start - (window - span), mid, NEG_BIG), last], axis=1)

        def finish(sc, item):
            top = jnp.max(sc, axis=-1, keepdims=True)
            e = jnp.exp2((sc - top) * factor)
            total = jnp.sum(e, axis=-1, keepdims=True)
            acc = jnp.dot(e.astype(jnp.bfloat16), kv[rows, item[1]], preferred_element_type=jnp.float32)
            return (acc / total).astype(jnp.bfloat16)

        def some(first):
            items = []
            for u in range(together):
                g = first + u
                for h in range(heads):
                    offsets = (g * head, width + g * head, (g * heads + h) * head)
                    items.append(tuple(pl.ds(o if isinstance(o, int) else pl.multiple_of(o, head), head) for o in offsets))
            ahead = scores(items[0])
            for k, item in enumerate(items):
                now = ahead
                if k + 1 < len(items):
                    ahead = scores(items[k + 1])
                q_s[s, :, item[2]] = finish(now, item)

        if together == groups:
            some(0)
        else:
            @pl.loop(0, groups // together)
            def _(i):
                some(i * together)

    tile = width
    loads = [pltpu.make_async_copy(x_hbm.at[block(s)], xn.at[s], xsem.at[s]) for s in range(2)]
    for cp in loads:
        cp.start()
    for i in range(kv_ring):
        kv_start(0, i)
    for i in range(q_ring):
        q_stage(0, i).start()
    barrier = pltpu.get_barrier_semaphore()
    for dev in (left, right) + peers[:2]:
        signal(barrier, dev)
    pl.semaphore_wait(barrier, 4)
    for s in range(2):
        loads[s].wait()
        x_copy(0, s).start()

    @pl.loop(0, kv_parts)
    def _(i):
        kv_wait(0, i)
        kv_flat(0, i)
        kv_next(0, i)

    @pl.loop(0, num_layers)
    def _(layer):
        slot = lax.rem(layer, 2)
        more = layer + 1 < num_layers
        chunk = lax.rem(me + layer + 1, num_dev)

        @pl.when(layer > 0)
        def _():
            for s in range(2):
                for j in range(2):
                    h_copy(s, j).wait_send()

            @pl.when(is_odd)
            def _():
                for s in range(2):
                    c_copy(s).wait_send()

        @pl.loop(0, 2)
        def _(s):
            with jax.named_scope("own_norm"):
                norm_into(xn.at[s])

            @pl.loop(0, 2)
            @scoped("own")
            def _(j):
                cols = pl.ds(pl.multiple_of(j * tile, tile), tile)
                kv[block(2 + s), cols] = dot(wkv_s[:, cols])

                @pl.when((layer > 0) & (s == 0) & (j == 0))
                def _():
                    pl.semaphore_wait(h_free, 1)

                    @pl.when(is_odd)
                    def _():
                        pl.semaphore_wait(c_free, 1)

                h_copy(s, j).start()

            @pl.when(is_odd)
            def _():
                c_copy(s).start()

        @pl.loop(0, q_parts)
        @scoped("q_lay")
        def _(i):
            q_stage(layer, i).wait()
            q_flat(layer, i)
            q_next(layer, i)

        wo_copy(layer).start()

        @pl.when(more)
        def _():
            for i in range(kv_ring):
                kv_start(layer + 1, i)

        @pl.loop(0, 2)
        def _(s):
            @pl.loop(jnp.where(is_odd, s, 2 * s), jnp.where(is_odd, s + 1, 2))
            def _(t):
                with jax.named_scope("x_wait"):
                    x_copy(slot, t).wait_recv()
                with jax.named_scope("norm"):
                    norm_into(xr.at[slot, t])

                @pl.loop(0, 2)
                @scoped("query")
                def _(j):
                    cols = pl.ds(pl.multiple_of(j * tile, tile), tile)
                    q_s[t, :, cols] = dot(wq_s[:, cols])

                @pl.when(is_odd)
                def _():
                    @pl.loop(0, 2)
                    @scoped("keys")
                    def _(j):
                        cols = pl.ds(pl.multiple_of(j * tile, tile), tile)
                        kv[block(4 + t), cols] = dot(wkv_s[:, cols])

            @pl.when(s == 0)
            @scoped("h_wait")
            def _():
                for i in range(2):
                    for j in range(2):
                        h_copy(i, j).wait_recv()

            @pl.when(is_even)
            @scoped("c_wait")
            def _():
                c_copy(s).wait_recv()

            for first, cond in ((2, chunk >= 2), (1, chunk == 1), (0, chunk == 0)):
                @pl.when(cond)
                @scoped("attend")
                def _():
                    attend(s, (2 * first + 1) * blk if first == 2 else (2 * first + 2) * blk, WINDOW - s * blk - first * 2 * blk)

            @pl.when((s == 1) & more)
            def _():
                signal(h_free, left)

                @pl.when(is_even)
                def _():
                    signal(c_free, right)

            out_tiles = 3
            out_tile = dim // out_tiles

            @pl.when(s == 0)
            def _():
                wo_copy(layer).wait()

            def out_dot(j):
                cols = pl.ds(pl.multiple_of(j * out_tile, out_tile), out_tile)
                upd_s[:, cols] = jnp.dot(q_s[s], wo_s[:, cols], preferred_element_type=jnp.float32)

            relay = (s == 1) & more

            @pl.when(relay)
            def _():
                @pl.loop(0, out_tiles)
                @scoped("out_lay")
                def _(j):
                    per = kv_parts // out_tiles
                    for t in range(per):
                        kv_wait(layer + 1, j * per + t)
                        kv_flat(layer + 1, j * per + t)
                        kv_next(layer + 1, j * per + t)
                    out_dot(j)

            @pl.when(jnp.logical_not(relay))
            def _():
                @pl.loop(0, out_tiles)
                @scoped("out")
                def _(j):
                    out_dot(j)

            with jax.named_scope("x_sent"):
                x_copy(slot, s).wait_send()
            step = min(16, blk)

            @pl.loop(0, blk // step, unroll=blk // step)
            def _(i):
                part = pl.ds(pl.multiple_of(i * step, step), step)
                upd = upd_s[part, :]
                scale = lax.rsqrt(jnp.mean(upd * upd, axis=-1, keepdims=True) + EPS_NORM)
                xn[s, part, :] = (xr[slot, s, part, :].astype(jnp.float32) + upd * scale).astype(jnp.bfloat16)

            @pl.when(more)
            def _():
                x_copy(1 - slot, s).start()

            @pl.when(jnp.logical_not(more))
            def _():
                keep(s).start()

                @pl.when(s == 0)
                def _():
                    for i in range(3):
                        g_copy(i, me).start()

    for s in range(2):
        for j in range(2):
            h_copy(s, j).wait_send()
        keep(s).wait()

    @pl.when(is_odd)
    def _():
        for s in range(2):
            c_copy(s).wait_send()

    for i in range(3):
        g_copy(i, me).wait_send()
        g_copy(i, sources[i]).wait_recv()


def window_stack(x, w_query, w_key, w_value, w_out, num_layers, num_dev):
    rows, dim = x.shape
    blk = rows // 2
    q_heads, head = w_query.shape[2:]
    kv_heads = w_key.shape[2]
    q_width, width = q_heads * head, kv_heads * head
    q_rows, q_ring, kv_rows, kv_ring = dim // 8, 4, dim // 9, 4
    any_ = pl.BlockSpec(memory_space=pl.ANY)
    bf = jnp.bfloat16
    dma, regular = pltpu.SemaphoreType.DMA, pltpu.SemaphoreType.REGULAR
    return pl.pallas_call(
        functools.partial(stack_kernel, num_dev, num_layers),
        in_specs=[any_] * 5,
        out_specs=any_,
        out_shape=jax.ShapeDtypeStruct((num_dev, rows, dim), bf),
        scratch_shapes=[
            pltpu.VMEM((2, 2, blk, dim), bf),
            pltpu.VMEM((2, blk, dim), bf),
            pltpu.VMEM((6 * blk, 2 * width), bf),
            pltpu.VMEM((blk, dim), bf),
            pltpu.VMEM((2, blk, q_width), bf),
            pltpu.VMEM((dim, q_width), bf),
            pltpu.VMEM((dim, 2 * width), bf),
            pltpu.VMEM((q_width, dim), bf),
            pltpu.VMEM((blk, dim), jnp.float32),
            pltpu.VMEM((q_ring, q_rows, q_heads, head), bf),
            pltpu.VMEM((kv_ring, kv_rows, kv_heads, head), bf),
            pltpu.VMEM((kv_ring, kv_rows, kv_heads, head), bf),
            dma((3,)), dma((3,)), dma((2,)), dma((2, 2)), dma((2, 2)), dma((2, 2)), dma((2,)), dma((2,)),
            regular, regular, dma((2,)), dma((q_ring,)), dma((kv_ring,)), dma((kv_ring,)), dma,
        ],
        compiler_params=pltpu.CompilerParams(vmem_limit_bytes=67043328, collective_id=2, has_side_effects=True),
        cost_estimate=pl.CostEstimate(flops=num_layers * 20 * 10 ** 9, bytes_accessed=num_layers * 28 * 10 ** 6, transcendentals=0),
        name="stack",
    )(x, w_query, w_key, w_value, w_out)


def norm_rows(src, dst):
    rows = src.shape[0]
    step = min(16, rows)

    @pl.loop(0, rows // step, unroll=min(16, rows // step))
    def _(i):
        part = pl.ds(pl.multiple_of(i * step, step), step)
        dst[part, :] = normed(src[part, :])


def gather_kernel(num_dev, layer, shift, x_in, wq_hbm, wk_hbm, wv_hbm, k_all, v_all, x_all, q_hbm, x_fin,
                  wq_st, wk_st, wv_st, wq_s, wk_s, wv_s, x_s, n_s, k_s, v_s, q_s, f_s, wsem, fsem, lsem, ssem, send, recv, psend, precv, csend, crecv):
    _, rows, dim = x_s.shape
    half = rows // 2
    me = lax.axis_index("cp")
    other = me + 1 - 2 * lax.rem(me, 2)
    near = (lax.rem(me + 2, num_dev), lax.rem(me + num_dev - 2, num_dev))
    hops = num_dev // 4

    def wrap(v):
        return lax.rem(v + 4 * num_dev, num_dev)

    def owner(dev, way, hop):
        if isinstance(way, int):
            return wrap(dev - 2 * hop) if way == 0 else wrap(dev + 2 * hop)
        return wrap(dev + jnp.where(way == 0, -2, 2) * hop)

    def piece(dev, h):
        return x_all.at[dev, pl.ds(h * half, half)]

    def link(way, hop, h):
        ref = piece(owner(me, way, hop - 1), h)
        return pltpu.make_async_remote_copy(src_ref=ref, dst_ref=ref, send_sem=send.at[way, hop, h], recv_sem=recv.at[way, hop, h],
                                            device_id={"cp": near[way]}, device_id_type=MESH)

    def landed(way, hop, h):
        ref = piece(owner(me, way, hop), h)
        return pltpu.make_async_remote_copy(src_ref=ref, dst_ref=ref, send_sem=send.at[way, hop, h], recv_sem=recv.at[way, hop, h],
                                            device_id={"cp": near[way]}, device_id_type=MESH)

    def across(way, hop, h, dev):
        ref = piece(owner(dev, way, hop), h)
        return pltpu.make_async_remote_copy(src_ref=ref, dst_ref=ref, send_sem=psend.at[way, hop, h], recv_sem=precv.at[way, hop, h],
                                            device_id={"cp": other}, device_id_type=MESH)

    crossings = [(0, 0, 1)] + [(way, hop, h) for hop in range(1, hops + 1) for way in range(2) for h in range(2) if hop < hops or way == h]

    def share(i, a, hop, chunk):
        src, dst = ((k_s, k_all), (v_s, v_all))[i]
        return pltpu.make_async_remote_copy(src_ref=src.at[a], dst_ref=dst.at[chunk], send_sem=csend.at[i, a], recv_sem=crecv.at[i, a, hop],
                                            device_id={"cp": other}, device_id_type=MESH)

    def finals():
        copies = []
        for i, block in enumerate((me, 2 * num_dev - 1 - me)):
            src = wrap(lax.div(block, 2) - shift)
            copies.append(pltpu.make_async_copy(piece(src, lax.rem(block, 2)), f_s.at[pl.ds(i * half, half)], fsem.at[i]))
        return copies

    wcopies = [pltpu.make_async_copy(w.at[layer], st, wsem.at[i]) for i, (w, st) in enumerate(((wk_hbm, wk_st), (wv_hbm, wv_st), (wq_hbm, wq_st)))]
    for cp in wcopies:
        cp.start()
    barrier = pltpu.get_barrier_semaphore()
    for dev in near + (other,):
        pl.semaphore_signal(barrier, inc=1, device_id={"cp": dev}, device_id_type=MESH)
    pl.semaphore_wait(barrier, 3)
    for way in range(2):
        link(way, 1, 1).start()
    across(0, 0, 1, me).start()
    for way in range(2):
        link(way, 2, 0).start()
        across(way, 1, 0, me).start()
    for cp in wcopies:
        cp.wait()
    step_rows = 256

    @pl.loop(0, dim // step_rows)
    def _(s):
        part = pl.ds(pl.multiple_of(s * step_rows, step_rows), step_rows)
        wk_s[part, :] = wk_st[part].reshape(step_rows, -1)
        wv_s[part, :] = wv_st[part].reshape(step_rows, -1)
        wq_s[part, :] = wq_st[part].reshape(step_rows, -1)

    @pl.loop(0, hops + 1)
    def _(hop):
        for h in range(2):
            for way in range(2):
                last_ok = way == h

                def arrive():
                    with jax.named_scope("land"):
                        landed(way, hop, h).wait_recv()
                    if last_ok:
                        @pl.when(hop < hops)
                        def _():
                            link(way, hop + 1, h).start()
                    else:
                        @pl.when(hop < hops - 1)
                        def _():
                            link(way, hop + 1, h).start()
                    across(way, hop, h, me).start()

                first_hop = 2 - h
                if last_ok:
                    pl.when(hop >= first_hop)(arrive)
                else:
                    pl.when((hop >= first_hop) & (hop < hops))(arrive)

        whole = (hop > 0) & (hop < hops)
        count = jnp.where(whole, 2, 1)

        def source(a):
            return wrap(me + jnp.where(a == 0, -2, 2) * hop)

        def load(a):
            return pltpu.make_async_copy(x_all.at[source(a)], x_s.at[a], lsem.at[a])

        load(0).start()

        @pl.loop(0, count)
        def _(a):
            with jax.named_scope("load"):
                load(a).wait()

            @pl.when(a + 1 < count)
            def _():
                load(a + 1).start()

            with jax.named_scope("norm"):
                norm_rows(x_s.at[a], n_s)
            chunk = wrap(source(a) + shift)

            def keep(i):
                src, dst = ((k_s, k_all), (v_s, v_all))[i]
                return pltpu.make_async_copy(src.at[a], dst.at[chunk], ssem.at[i, a])

            with jax.named_scope("keys"):
                k_s[a] = jnp.dot(n_s[...], wk_s[...], preferred_element_type=jnp.float32).astype(jnp.bfloat16)
            keep(0).start()
            share(0, a, hop, chunk).start()

            @pl.when(hop == hops)
            @scoped("cross")
            def _():
                for way, far, h in crossings:
                    across(way, far, h, other).wait_recv()
                for cp in finals():
                    cp.start()

            with jax.named_scope("keys"):
                v_s[a] = jnp.dot(n_s[...], wv_s[...], preferred_element_type=jnp.float32).astype(jnp.bfloat16)
            keep(1).start()
            share(1, a, hop, chunk).start()

        @pl.loop(0, count)
        def _(a):
            for i in range(2):
                src, dst = ((k_s, k_all), (v_s, v_all))[i]
                pltpu.make_async_copy(src.at[a], dst.at[wrap(source(a) + shift)], ssem.at[i, a]).wait()

                @pl.when(hop < hops)
                @scoped("shared")
                def _():
                    share(i, a, hop, wrap(source(a) + shift)).wait_send()

    for cp in finals():
        cp.wait()
    keep = pltpu.make_async_copy(f_s, x_fin, lsem.at[0])
    keep.start()
    norm_rows(f_s, n_s)
    with jax.named_scope("query"):
        q_s[...] = jnp.dot(n_s[...], wq_s[...], preferred_element_type=jnp.float32).astype(jnp.bfloat16)
    last = pltpu.make_async_copy(q_s, q_hbm, lsem.at[1])
    last.start()
    last.wait()
    keep.wait()
    for i in range(2):
        share(i, 0, hops, wrap(me + shift)).wait_send()
        for hop in range(hops + 1):
            for way in range(2 if 0 < hop < hops else 1):
                share(i, way, hop, wrap(owner(other, way, hop) + shift)).wait_recv()
    for way, hop, h in crossings:
        across(way, hop, h, me).wait_send()
        if hop + h > 1:
            link(way, hop, h).wait_send()


def gather_keys(x_all, w_query, w_key, w_value, layer, shift, num_dev):
    _, rows, dim = x_all.shape
    shapes = [w.shape[2:] for w in (w_query, w_key, w_value)]
    q_width, width = (h * e for h, e in shapes[:2])
    hops = num_dev // 4
    any_ = pl.BlockSpec(memory_space=pl.ANY)
    bf = jnp.bfloat16
    sem = pltpu.SemaphoreType.DMA
    seq = [jax.ShapeDtypeStruct((num_dev, rows, n), bf) for n in (width, width, dim)]
    own = [jax.ShapeDtypeStruct((rows, n), bf) for n in (q_width, dim)]
    return pl.pallas_call(
        functools.partial(gather_kernel, num_dev, layer, shift),
        in_specs=[any_] * 4,
        out_specs=[any_] * 5,
        out_shape=seq + own,
        input_output_aliases={0: 2},
        scratch_shapes=[pltpu.VMEM((dim,) + s, bf) for s in shapes] + [pltpu.VMEM((dim, n), bf) for n in (q_width, width, width)]
        + [pltpu.VMEM((2, rows, dim), bf), pltpu.VMEM((rows, dim), bf)] + [pltpu.VMEM((2, rows, width), bf)] * 2 + [pltpu.VMEM((rows, q_width), bf), pltpu.VMEM((rows, dim), bf)]
        + [sem((3,)), sem((2,)), sem((2,)), sem((2, 2))] + [sem((2, hops + 1, 2))] * 4 + [sem((2, 2)), sem((2, 2, hops + 1))],
        compiler_params=params(collective_id=1, has_side_effects=True),
        cost_estimate=pl.CostEstimate(flops=4 * rows * num_dev * dim * width, bytes_accessed=4 * dim * width, transcendentals=0),
        name="gather",
    )(x_all, w_query, w_key, w_value)


def causal_kernel(layer, seq, blk_ref, q_ref, k_ref, v_ref, x_ref, w_hbm, out_ref, o_s, w_s, upd_s, acc_s, top_s, tot_s, sem):
    g = pl.program_id(0)
    wcopy = pltpu.make_async_copy(w_hbm.at[layer], w_s, sem)

    @pl.when(g == 0)
    def _():
        wcopy.start()

    lead, trail = blk_ref[0], blk_ref[1]
    tile = 4 * BLK
    lanes = tot_s.shape[-1]
    per = tile // BLK
    front = seq // 2 // tile
    num_trail = lax.div(trail + 1 + per - 1, per) - front
    factor = LOG2_E * BLK ** -0.5
    def scores(item):
        _, qrow, t, limit, h = item
        q = q_ref[pl.ds(qrow, BLK), h * BLK:(h + 1) * BLK]
        s = lax.dot_general(q, k_ref[pl.ds(t, tile), :], (((1,), (1,)), ((), ())), preferred_element_type=jnp.float32)
        if limit is not None:
            reach = lax.broadcasted_iota(jnp.int32, (BLK, 1), 0) + limit
            s = jnp.where(lax.broadcasted_iota(jnp.int32, s.shape, 1) <= reach, s, NEG_BIG)
        return s

    def finish(s, item):
        slot, _, t, _, h = item
        top = jnp.max(s, axis=-1, keepdims=True)
        e = jnp.exp2((s - top) * factor)
        tot_s[slot, h] = functools.reduce(jnp.add, [e[:, i * lanes:(i + 1) * lanes] for i in range(tile // lanes)])
        acc_s[slot, h] = jnp.dot(e.astype(jnp.bfloat16), v_ref[pl.ds(t, tile), :], preferred_element_type=jnp.float32)
        top_s[slot, h] = top

    items = []
    for j in range(front):
        chains = [(j, BLK, j * tile, None)]
        if j < 2:
            block, t = ((trail, front + num_trail - 1), (lead, front - num_trail))[j]
            t = pl.multiple_of(t * tile, tile)
            chains.append((front + j, (1 - j) * BLK, t, block * BLK - t))
        if j > 0:
            late = j < num_trail
            t = jnp.where(late, front + j - 1, j - num_trail) * tile
            chains.append((front + 1 + j, pl.multiple_of(jnp.where(late, BLK, 0), BLK), pl.multiple_of(t, tile), None))
        for chain in chains:
            items += [chain + (h,) for h in range(2)]
    ready = scores(items[0])
    for i, item in enumerate(items):
        now = ready
        if i + 1 < len(items):
            ready = scores(items[i + 1])
        finish(now, item)

    for h in range(2):
        cols = pl.ds(pl.multiple_of(g * 2 * BLK + h * BLK, BLK), BLK)
        shared = range(front + 2, 2 * front + 1)
        for i, slots in enumerate(([front + 1, *shared], [*range(front + 1), *shared])):
            tops = []
            for slot in slots:
                top = top_s[slot, h]
                if slot > front + 1:
                    late = slot - front - 1 < num_trail
                    top = jnp.where(late if i == 1 else jnp.logical_not(late), top, NEG_BIG)
                tops.append(top)
            new = functools.reduce(jnp.maximum, tops)
            acc = total = None
            for slot, top in zip(slots, tops):
                fix = jnp.exp2((top - new) * factor)
                a, b = acc_s[slot, h] * fix, tot_s[slot, h] * fix
                acc, total = (a, b) if acc is None else (acc + a, total + b)
            o_s[i * BLK:(i + 1) * BLK, cols] = (acc / jnp.sum(total, axis=-1, keepdims=True)).astype(jnp.bfloat16)

    @pl.when(g == pl.num_programs(0) - 1)
    def _():
        wcopy.wait()
        output_rows(o_s, w_s, x_ref, out_ref, upd_s)


def causal_layer(blocks, q, k_all, v_all, x, w_out, layer):
    rows, dim = x.shape
    seq = k_all.shape[0]
    slots = 2 * (seq // 2 // (4 * BLK)) + 1
    kv = pl.BlockSpec((seq, BLK), lambda g, b: (0, g))
    row = pl.BlockSpec((rows, dim), lambda g, b: (0, 0))
    return pl.pallas_call(
        functools.partial(causal_kernel, layer, seq),
        grid_spec=pltpu.PrefetchScalarGridSpec(
            num_scalar_prefetch=1,
            grid=(k_all.shape[1] // BLK,),
            in_specs=[pl.BlockSpec((rows, 2 * BLK), lambda g, b: (0, g)), kv, kv, row, pl.BlockSpec(memory_space=pl.ANY)],
            out_specs=row,
            scratch_shapes=[
                pltpu.VMEM(q.shape, jnp.bfloat16),
                pltpu.VMEM(w_out.shape[1:], jnp.bfloat16),
                pltpu.VMEM((rows, dim), jnp.float32),
                pltpu.VMEM((slots, 2, BLK, BLK), jnp.float32),
                pltpu.VMEM((slots, 2, BLK, 1), jnp.float32),
                pltpu.VMEM((slots, 2, BLK, 128), jnp.float32),
                pltpu.SemaphoreType.DMA,
            ],
        ),
        out_shape=jax.ShapeDtypeStruct((rows, dim), jnp.bfloat16),
        compiler_params=params(),
        cost_estimate=pl.CostEstimate(flops=30 * 10 ** 9, bytes_accessed=2 * w_out[0].size, transcendentals=0),
        name="causal",
    )(blocks, q, k_all, v_all, x, w_out)


def solution(mesh):
    num_dev = mesh.shape["cp"]

    def per_device(hidden, w_query, w_key, w_value, w_out):
        rank = lax.axis_index("cp")
        num_layers = w_query.shape[0]
        rows, dim = hidden.shape
        w_out = w_out.reshape(num_layers, -1, dim)
        last = num_layers - 1
        x = window_stack(hidden, w_query, w_key, w_value, w_out, last, num_dev)
        k_all, v_all, _, q, x_fin = gather_keys(x, w_query, w_key, w_value, last, last, num_dev)
        blocks = jnp.stack([rank, 2 * num_dev - 1 - rank]).astype(jnp.int32)
        return causal_layer(blocks, q, k_all.reshape(-1, k_all.shape[-1]), v_all.reshape(-1, v_all.shape[-1]), x_fin, w_out, last)

    row_spec = P(("dp", "cp"), None)
    return jax.shard_map(per_device, mesh=mesh, in_specs=(row_spec, P(), P(), P(), P()), out_specs=row_spec, check_vma=False)
```

```python
import functools

import jax
import jax.numpy as jnp
from jax import lax
from jax.experimental import pallas as pl
from jax.experimental.pallas import tpu as pltpu
from jax.sharding import PartitionSpec as P

WINDOW = 1024
EPS_NORM = 1e-6
NEG_BIG = -1e30
LOG2_E = 1.4426950408889634
BLK = 256
VMEM_BYTES = 62 << 20
MESH = pl.DeviceIdType.MESH


def params(**kw):
    return pltpu.CompilerParams(vmem_limit_bytes=VMEM_BYTES, **kw)


def normed(rows):
    wide = rows.astype(jnp.float32)
    return (wide * lax.rsqrt(jnp.mean(wide * wide, axis=-1, keepdims=True) + EPS_NORM)).astype(jnp.bfloat16)


def output_rows(o_s, w_s, x_ref, out_ref, upd_s):
    rows, dim = x_ref.shape
    tile = 768

    @pl.loop(0, dim // tile)
    def _(s):
        cols = pl.ds(pl.multiple_of(s * tile, tile), tile)
        upd_s[:, cols] = jnp.dot(o_s[...], w_s[:, cols], preferred_element_type=jnp.float32)

    @pl.loop(0, rows // 16, unroll=16)
    def _(s):
        part = pl.ds(pl.multiple_of(s * 16, 16), 16)
        upd = upd_s[part, :]
        scale = lax.rsqrt(jnp.mean(upd * upd, axis=-1, keepdims=True) + EPS_NORM)
        out_ref[part, :] = (x_ref[part, :].astype(jnp.float32) + upd * scale).astype(jnp.bfloat16)


def scoped(name):
    def wrap(fn):
        def run(*args):
            with jax.named_scope(name):
                return fn(*args)

        return run

    return wrap


def stack_kernel(num_dev, num_layers, x_hbm, wq_hbm, wk_hbm, wv_hbm, wo_hbm, x_all,
                 xr, xn, kv, n_s, q_s, wq_s, wkv_s, wo_s, upd_s, stq, stk, stv,
                 g_send, g_recv, x_send, x_recv, h_send, h_recv, c_send, c_recv, h_free, c_free, xsem, qsem, ksem, vsem, wsem):
    blk, dim = n_s.shape
    width = wkv_s.shape[1] // 2
    heads = q_s.shape[2] // width
    head = BLK
    q_rows, kv_rows = stq.shape[1], stk.shape[1]
    q_ring, kv_ring = stq.shape[0], stk.shape[0]
    q_parts, kv_parts = dim // q_rows, dim // kv_rows
    me = lax.axis_index("cp")
    odd = lax.rem(me, 2)
    is_odd, is_even = odd == 1, odd == 0
    left, right = lax.rem(me + num_dev - 1, num_dev), lax.rem(me + 1, num_dev)

    other = jnp.where(is_odd, left, right)
    peers = (lax.rem(me + 2, num_dev), lax.rem(me + num_dev - 2, num_dev), other)
    sources = (peers[1], peers[0], other)

    def block(i):
        return pl.ds(pl.multiple_of(i * blk, blk), blk)

    def remote(src, dst, send, recv, dev):
        return pltpu.make_async_remote_copy(src_ref=src, dst_ref=dst, send_sem=send, recv_sem=recv, device_id={"cp": dev}, device_id_type=MESH)

    def x_copy(slot, s):
        return remote(xn.at[s], xr.at[slot, s], x_send.at[s], x_recv.at[slot, s], left)

    def g_copy(i, owner):
        return remote(xn.at[0], x_all.at[owner, block(0)], g_send.at[i], g_recv.at[i], peers[i])

    def keep(s):
        return pltpu.make_async_copy(xn.at[s], x_all.at[me, block(s)], xsem.at[s])

    def h_copy(s, j):
        cols = pl.ds(pl.multiple_of(j * width, width), width)
        return remote(kv.at[block(2 + s), cols], kv.at[block(s), cols], h_send.at[s, j], h_recv.at[s, j], right)

    def c_copy(s):
        return remote(kv.at[block(2 + s)], kv.at[block(4 + s)], c_send.at[s], c_recv.at[s], left)

    def signal(sem, dev):
        pl.semaphore_signal(sem, inc=1, device_id={"cp": dev}, device_id_type=MESH)

    def q_stage(layer, i):
        b = lax.rem(layer * q_parts + i, q_ring)
        return pltpu.make_async_copy(wq_hbm.at[layer, pl.ds(i * q_rows, q_rows)], stq.at[b], qsem.at[b])

    def kv_stage(layer, i):
        b = lax.rem(layer * kv_parts + i, kv_ring)
        rows = pl.ds(i * kv_rows, kv_rows)
        return (pltpu.make_async_copy(wk_hbm.at[layer, rows], stk.at[b], ksem.at[b]),
                pltpu.make_async_copy(wv_hbm.at[layer, rows], stv.at[b], vsem.at[b]))

    def kv_start(layer, i):
        for cp in kv_stage(layer, i):
            cp.start()

    def kv_wait(layer, i):
        for cp in kv_stage(layer, i):
            cp.wait()

    def kv_flat(layer, i):
        b = lax.rem(layer * kv_parts + i, kv_ring)
        rows = pl.ds(pl.multiple_of(i * kv_rows, 16), kv_rows)
        wkv_s[rows, :width] = stk[b].reshape(kv_rows, width)
        wkv_s[rows, width:] = stv[b].reshape(kv_rows, width)

    def q_flat(layer, i):
        b = lax.rem(layer * q_parts + i, q_ring)
        wq_s[pl.ds(pl.multiple_of(i * q_rows, 16), q_rows), :] = stq[b].reshape(q_rows, wq_s.shape[1])

    def kv_next(layer, i):
        @pl.when(i + kv_ring < kv_parts)
        def _():
            kv_start(layer, i + kv_ring)

    def q_next(layer, i):
        after = i + q_ring

        @pl.when(after < q_parts)
        def _():
            q_stage(layer, after).start()

        @pl.when((after >= q_parts) & (layer + 1 < num_layers))
        def _():
            q_stage(layer + 1, after - q_parts).start()

    def wo_copy(layer):
        return pltpu.make_async_copy(wo_hbm.at[layer], wo_s, wsem)

    def norm_into(ref):
        step = min(16, blk)

        @pl.loop(0, blk // step, unroll=blk // step)
        def _(i):
            part = pl.ds(pl.multiple_of(i * step, step), step)
            n_s[part, :] = normed(ref[part, :])

    def dot(w):
        return jnp.dot(n_s[...], w, preferred_element_type=jnp.float32).astype(jnp.bfloat16)

    def attend(s, span, start):
        window = WINDOW + blk
        rows = pl.ds(pl.multiple_of(s * blk + window - span, blk), span)
        factor = LOG2_E * head ** -0.5
        groups = width // head
        together = groups if span == window else 2
        qi = lax.broadcasted_iota(jnp.int32, (blk, blk), 0)
        ki = lax.broadcasted_iota(jnp.int32, (blk, blk), 1)

        def scores(item):
            sc = lax.dot_general(q_s[s, :, item[2]], kv[rows, item[0]], (((1,), (1,)), ((), ())), preferred_element_type=jnp.float32)
            last = jnp.where(ki <= qi, sc[:, span - blk:], NEG_BIG)
            if span == window:
                return jnp.concatenate([jnp.where(ki > qi, sc[:, :blk], NEG_BIG), sc[:, blk:span - blk], last], axis=1)
            mid = sc[:, :span - blk]
            pos = lax.broadcasted_iota(jnp.int32, mid.shape, 1)
            return jnp.concatenate([jnp.where(pos >= start - (window - span), mid, NEG_BIG), last], axis=1)

        def finish(sc, item):
            top = jnp.max(sc, axis=-1, keepdims=True)
            e = jnp.exp2((sc - top) * factor)
            total = jnp.sum(e, axis=-1, keepdims=True)
            acc = jnp.dot(e.astype(jnp.bfloat16), kv[rows, item[1]], preferred_element_type=jnp.float32)
            return (acc / total).astype(jnp.bfloat16)

        def some(first):
            items = []
            for u in range(together):
                g = first + u
                for h in range(heads):
                    offsets = (g * head, width + g * head, (g * heads + h) * head)
                    items.append(tuple(pl.ds(o if isinstance(o, int) else pl.multiple_of(o, head), head) for o in offsets))
            ahead = scores(items[0])
            for k, item in enumerate(items):
                now = ahead
                if k + 1 < len(items):
                    ahead = scores(items[k + 1])
                q_s[s, :, item[2]] = finish(now, item)

        if together == groups:
            some(0)
        else:
            @pl.loop(0, groups // together)
            def _(i):
                some(i * together)

    tile = width
    loads = [pltpu.make_async_copy(x_hbm.at[block(s)], xn.at[s], xsem.at[s]) for s in range(2)]
    for cp in loads:
        cp.start()
    for i in range(kv_ring):
        kv_start(0, i)
    for i in range(q_ring):
        q_stage(0, i).start()
    barrier = pltpu.get_barrier_semaphore()
    for dev in (left, right) + peers[:2]:
        signal(barrier, dev)
    pl.semaphore_wait(barrier, 4)
    for s in range(2):
        loads[s].wait()
        x_copy(0, s).start()

    @pl.loop(0, kv_parts)
    def _(i):
        kv_wait(0, i)
        kv_flat(0, i)
        kv_next(0, i)

    @pl.loop(0, num_layers)
    def _(layer):
        slot = lax.rem(layer, 2)
        more = layer + 1 < num_layers
        chunk = lax.rem(me + layer + 1, num_dev)

        @pl.when(layer > 0)
        def _():
            for s in range(2):
                for j in range(2):
                    h_copy(s, j).wait_send()

            @pl.when(is_odd)
            def _():
                for s in range(2):
                    c_copy(s).wait_send()

        @pl.loop(0, 2)
        def _(s):
            with jax.named_scope("own_norm"):
                norm_into(xn.at[s])

            @pl.loop(0, 2)
            @scoped("own")
            def _(j):
                cols = pl.ds(pl.multiple_of(j * tile, tile), tile)
                kv[block(2 + s), cols] = dot(wkv_s[:, cols])

                @pl.when((layer > 0) & (s == 0) & (j == 0))
                def _():
                    pl.semaphore_wait(h_free, 1)

                    @pl.when(is_odd)
                    def _():
                        pl.semaphore_wait(c_free, 1)

                h_copy(s, j).start()

            @pl.when(is_odd)
            def _():
                c_copy(s).start()

        @pl.loop(0, q_parts)
        @scoped("q_lay")
        def _(i):
            q_stage(layer, i).wait()
            q_flat(layer, i)
            q_next(layer, i)

        wo_copy(layer).start()

        @pl.when(more)
        def _():
            for i in range(kv_ring):
                kv_start(layer + 1, i)

        @pl.loop(0, 2)
        def _(s):
            @pl.loop(jnp.where(is_odd, s, 2 * s), jnp.where(is_odd, s + 1, 2))
            def _(t):
                with jax.named_scope("x_wait"):
                    x_copy(slot, t).wait_recv()
                with jax.named_scope("norm"):
                    norm_into(xr.at[slot, t])

                @pl.loop(0, 2)
                @scoped("query")
                def _(j):
                    cols = pl.ds(pl.multiple_of(j * tile, tile), tile)
                    q_s[t, :, cols] = dot(wq_s[:, cols])

                @pl.when(is_odd)
                def _():
                    @pl.loop(0, 2)
                    @scoped("keys")
                    def _(j):
                        cols = pl.ds(pl.multiple_of(j * tile, tile), tile)
                        kv[block(4 + t), cols] = dot(wkv_s[:, cols])

            @pl.when(s == 0)
            @scoped("h_wait")
            def _():
                for i in range(2):
                    for j in range(2):
                        h_copy(i, j).wait_recv()

            @pl.when(is_even)
            @scoped("c_wait")
            def _():
                c_copy(s).wait_recv()

            for first, cond in ((2, chunk >= 2), (1, chunk == 1), (0, chunk == 0)):
                @pl.when(cond)
                @scoped("attend")
                def _():
                    attend(s, (2 * first + 1) * blk if first == 2 else (2 * first + 2) * blk, WINDOW - s * blk - first * 2 * blk)

            @pl.when((s == 1) & more)
            def _():
                signal(h_free, left)

                @pl.when(is_even)
                def _():
                    signal(c_free, right)

            out_tiles = 3
            out_tile = dim // out_tiles

            @pl.when(s == 0)
            def _():
                wo_copy(layer).wait()

            def out_dot(j):
                cols = pl.ds(pl.multiple_of(j * out_tile, out_tile), out_tile)
                upd_s[:, cols] = jnp.dot(q_s[s], wo_s[:, cols], preferred_element_type=jnp.float32)

            relay = (s == 1) & more

            @pl.when(relay)
            def _():
                @pl.loop(0, out_tiles)
                @scoped("out_lay")
                def _(j):
                    per = kv_parts // out_tiles
                    for t in range(per):
                        kv_wait(layer + 1, j * per + t)
                        kv_flat(layer + 1, j * per + t)
                        kv_next(layer + 1, j * per + t)
                    out_dot(j)

            @pl.when(jnp.logical_not(relay))
            def _():
                @pl.loop(0, out_tiles)
                @scoped("out")
                def _(j):
                    out_dot(j)

            with jax.named_scope("x_sent"):
                x_copy(slot, s).wait_send()
            step = min(16, blk)

            @pl.loop(0, blk // step, unroll=blk // step)
            def _(i):
                part = pl.ds(pl.multiple_of(i * step, step), step)
                upd = upd_s[part, :]
                scale = lax.rsqrt(jnp.mean(upd * upd, axis=-1, keepdims=True) + EPS_NORM)
                xn[s, part, :] = (xr[slot, s, part, :].astype(jnp.float32) + upd * scale).astype(jnp.bfloat16)

            @pl.when(more)
            def _():
                x_copy(1 - slot, s).start()

            @pl.when(jnp.logical_not(more))
            def _():
                keep(s).start()

                @pl.when(s == 0)
                def _():
                    for i in range(3):
                        g_copy(i, me).start()

    for s in range(2):
        for j in range(2):
            h_copy(s, j).wait_send()
        keep(s).wait()

    @pl.when(is_odd)
    def _():
        for s in range(2):
            c_copy(s).wait_send()

    for i in range(3):
        g_copy(i, me).wait_send()
        g_copy(i, sources[i]).wait_recv()


def window_stack(x, w_query, w_key, w_value, w_out, num_layers, num_dev):
    rows, dim = x.shape
    blk = rows // 2
    q_heads, head = w_query.shape[2:]
    kv_heads = w_key.shape[2]
    q_width, width = q_heads * head, kv_heads * head
    q_rows, q_ring, kv_rows, kv_ring = dim // 8, 4, dim // 9, 4
    any_ = pl.BlockSpec(memory_space=pl.ANY)
    bf = jnp.bfloat16
    dma, regular = pltpu.SemaphoreType.DMA, pltpu.SemaphoreType.REGULAR
    return pl.pallas_call(
        functools.partial(stack_kernel, num_dev, num_layers),
        in_specs=[any_] * 5,
        out_specs=any_,
        out_shape=jax.ShapeDtypeStruct((num_dev, rows, dim), bf),
        scratch_shapes=[
            pltpu.VMEM((2, 2, blk, dim), bf),
            pltpu.VMEM((2, blk, dim), bf),
            pltpu.VMEM((6 * blk, 2 * width), bf),
            pltpu.VMEM((blk, dim), bf),
            pltpu.VMEM((2, blk, q_width), bf),
            pltpu.VMEM((dim, q_width), bf),
            pltpu.VMEM((dim, 2 * width), bf),
            pltpu.VMEM((q_width, dim), bf),
            pltpu.VMEM((blk, dim), jnp.float32),
            pltpu.VMEM((q_ring, q_rows, q_heads, head), bf),
            pltpu.VMEM((kv_ring, kv_rows, kv_heads, head), bf),
            pltpu.VMEM((kv_ring, kv_rows, kv_heads, head), bf),
            dma((3,)), dma((3,)), dma((2,)), dma((2, 2)), dma((2, 2)), dma((2, 2)), dma((2,)), dma((2,)),
            regular, regular, dma((2,)), dma((q_ring,)), dma((kv_ring,)), dma((kv_ring,)), dma,
        ],
        compiler_params=pltpu.CompilerParams(vmem_limit_bytes=67043328, collective_id=2, has_side_effects=True),
        cost_estimate=pl.CostEstimate(flops=num_layers * 20 * 10 ** 9, bytes_accessed=num_layers * 28 * 10 ** 6, transcendentals=0),
        name="stack",
    )(x, w_query, w_key, w_value, w_out)


def norm_rows(src, dst):
    rows = src.shape[0]
    step = min(16, rows)

    @pl.loop(0, rows // step, unroll=min(16, rows // step))
    def _(i):
        part = pl.ds(pl.multiple_of(i * step, step), step)
        dst[part, :] = normed(src[part, :])


def gather_kernel(num_dev, layer, shift, x_in, wq_hbm, wk_hbm, wv_hbm, k_all, v_all, x_all, q_hbm, x_fin,
                  wq_st, wk_st, wv_st, wq_s, wk_s, wv_s, x_s, n_s, k_s, v_s, q_s, f_s, wsem, fsem, lsem, ssem, send, recv, psend, precv, csend, crecv):
    _, rows, dim = x_s.shape
    half = rows // 2
    me = lax.axis_index("cp")
    other = me + 1 - 2 * lax.rem(me, 2)
    near = (lax.rem(me + 2, num_dev), lax.rem(me + num_dev - 2, num_dev))
    hops = num_dev // 4

    def wrap(v):
        return lax.rem(v + 4 * num_dev, num_dev)

    def owner(dev, way, hop):
        if isinstance(way, int):
            return wrap(dev - 2 * hop) if way == 0 else wrap(dev + 2 * hop)
        return wrap(dev + jnp.where(way == 0, -2, 2) * hop)

    def piece(dev, h):
        return x_all.at[dev, pl.ds(h * half, half)]

    def link(way, hop, h):
        ref = piece(owner(me, way, hop - 1), h)
        return pltpu.make_async_remote_copy(src_ref=ref, dst_ref=ref, send_sem=send.at[way, hop, h], recv_sem=recv.at[way, hop, h],
                                            device_id={"cp": near[way]}, device_id_type=MESH)

    def landed(way, hop, h):
        ref = piece(owner(me, way, hop), h)
        return pltpu.make_async_remote_copy(src_ref=ref, dst_ref=ref, send_sem=send.at[way, hop, h], recv_sem=recv.at[way, hop, h],
                                            device_id={"cp": near[way]}, device_id_type=MESH)

    def across(way, hop, h, dev):
        ref = piece(owner(dev, way, hop), h)
        return pltpu.make_async_remote_copy(src_ref=ref, dst_ref=ref, send_sem=psend.at[way, hop, h], recv_sem=precv.at[way, hop, h],
                                            device_id={"cp": other}, device_id_type=MESH)

    crossings = [(0, 0, 1)] + [(way, hop, h) for hop in range(1, hops + 1) for way in range(2) for h in range(2) if hop < hops or way == h]

    def share(i, a, hop, chunk):
        src, dst = ((k_s, k_all), (v_s, v_all))[i]
        return pltpu.make_async_remote_copy(src_ref=src.at[a], dst_ref=dst.at[chunk], send_sem=csend.at[i, a], recv_sem=crecv.at[i, a, hop],
                                            device_id={"cp": other}, device_id_type=MESH)

    def kept(i):
        block = jnp.where(i == 0, me, 2 * num_dev - 1 - me)
        return wrap(lax.div(block, 2) - shift), block

    def early(i):
        return lax.div(kept(i)[0], 2) != lax.rem(lax.div(me, 2) + hops, num_dev // 2)

    def final(i):
        src, block = kept(i)
        return pltpu.make_async_copy(piece(src, lax.rem(block, 2)), f_s.at[pl.ds(i * half, half)], fsem.at[i])

    def queries(i):
        part = pl.ds(pl.multiple_of(i * half, half), half)
        final(i).wait()
        norm_rows(f_s.at[part], n_s.at[pl.ds(0, half)])
        with jax.named_scope("query"):
            q_s[part, :] = jnp.dot(n_s[:half], wq_s[...], preferred_element_type=jnp.float32).astype(jnp.bfloat16)

    wcopies = [pltpu.make_async_copy(w.at[layer], st, wsem.at[i]) for i, (w, st) in enumerate(((wk_hbm, wk_st), (wv_hbm, wv_st), (wq_hbm, wq_st)))]
    for cp in wcopies:
        cp.start()
    barrier = pltpu.get_barrier_semaphore()
    for dev in near + (other,):
        pl.semaphore_signal(barrier, inc=1, device_id={"cp": dev}, device_id_type=MESH)
    pl.semaphore_wait(barrier, 3)
    for way in range(2):
        link(way, 1, 1).start()
    across(0, 0, 1, me).start()
    for way in range(2):
        link(way, 2, 0).start()
        across(way, 1, 0, me).start()
    for cp in wcopies:
        cp.wait()
    step_rows = 256

    @pl.loop(0, dim // step_rows)
    def _(s):
        part = pl.ds(pl.multiple_of(s * step_rows, step_rows), step_rows)
        wk_s[part, :] = wk_st[part].reshape(step_rows, -1)
        wv_s[part, :] = wv_st[part].reshape(step_rows, -1)
        wq_s[part, :] = wq_st[part].reshape(step_rows, -1)

    @pl.loop(0, hops + 1)
    def _(hop):
        @pl.when(hop == hops)
        def _():
            for way, far, h in crossings:
                if far < hops:
                    across(way, far, h, other).wait_recv()
            for i in range(2):
                pl.when(early(i))(final(i).start)

            @pl.loop(0, 2)
            def _(i):
                @pl.when(early(i))
                def _():
                    queries(i)

        for h in range(2):
            for way in range(2):
                last_ok = way == h

                def arrive():
                    with jax.named_scope("land"):
                        landed(way, hop, h).wait_recv()
                    if last_ok:
                        @pl.when(hop < hops)
                        def _():
                            link(way, hop + 1, h).start()
                    else:
                        @pl.when(hop < hops - 1)
                        def _():
                            link(way, hop + 1, h).start()
                    across(way, hop, h, me).start()

                first_hop = 2 - h
                if last_ok:
                    pl.when(hop >= first_hop)(arrive)
                else:
                    pl.when((hop >= first_hop) & (hop < hops))(arrive)

        whole = (hop > 0) & (hop < hops)
        count = jnp.where(whole, 2, 1)

        def source(a):
            return wrap(me + jnp.where(a == 0, -2, 2) * hop)

        def load(a):
            return pltpu.make_async_copy(x_all.at[source(a)], x_s.at[a], lsem.at[a])

        load(0).start()

        @pl.loop(0, count)
        def _(a):
            with jax.named_scope("load"):
                load(a).wait()

            @pl.when(a + 1 < count)
            def _():
                load(a + 1).start()

            with jax.named_scope("norm"):
                norm_rows(x_s.at[a], n_s)
            chunk = wrap(source(a) + shift)

            def keep(i):
                src, dst = ((k_s, k_all), (v_s, v_all))[i]
                return pltpu.make_async_copy(src.at[a], dst.at[chunk], ssem.at[i, a])

            with jax.named_scope("keys"):
                k_s[a] = jnp.dot(n_s[...], wk_s[...], preferred_element_type=jnp.float32).astype(jnp.bfloat16)
            keep(0).start()
            share(0, a, hop, chunk).start()

            @pl.when(hop == hops)
            @scoped("cross")
            def _():
                for way in range(2):
                    across(way, hops, way, other).wait_recv()
                for i in range(2):
                    pl.when(jnp.logical_not(early(i)))(final(i).start)

            with jax.named_scope("keys"):
                v_s[a] = jnp.dot(n_s[...], wv_s[...], preferred_element_type=jnp.float32).astype(jnp.bfloat16)
            keep(1).start()
            share(1, a, hop, chunk).start()

        @pl.loop(0, count)
        def _(a):
            for i in range(2):
                src, dst = ((k_s, k_all), (v_s, v_all))[i]
                pltpu.make_async_copy(src.at[a], dst.at[wrap(source(a) + shift)], ssem.at[i, a]).wait()

                @pl.when(hop < hops)
                @scoped("shared")
                def _():
                    share(i, a, hop, wrap(source(a) + shift)).wait_send()

    @pl.loop(0, 2)
    def _(i):
        @pl.when(jnp.logical_not(early(i)))
        def _():
            queries(i)

    keep = pltpu.make_async_copy(f_s, x_fin, lsem.at[0])
    keep.start()
    last = pltpu.make_async_copy(q_s, q_hbm, lsem.at[1])
    last.start()
    last.wait()
    keep.wait()
    for i in range(2):
        share(i, 0, hops, wrap(me + shift)).wait_send()
        for hop in range(hops + 1):
            for way in range(2 if 0 < hop < hops else 1):
                share(i, way, hop, wrap(owner(other, way, hop) + shift)).wait_recv()
    for way, hop, h in crossings:
        across(way, hop, h, me).wait_send()
        if hop + h > 1:
            link(way, hop, h).wait_send()


def gather_keys(x_all, w_query, w_key, w_value, layer, shift, num_dev):
    _, rows, dim = x_all.shape
    shapes = [w.shape[2:] for w in (w_query, w_key, w_value)]
    q_width, width = (h * e for h, e in shapes[:2])
    hops = num_dev // 4
    any_ = pl.BlockSpec(memory_space=pl.ANY)
    bf = jnp.bfloat16
    sem = pltpu.SemaphoreType.DMA
    seq = [jax.ShapeDtypeStruct((num_dev, rows, n), bf) for n in (width, width, dim)]
    own = [jax.ShapeDtypeStruct((rows, n), bf) for n in (q_width, dim)]
    return pl.pallas_call(
        functools.partial(gather_kernel, num_dev, layer, shift),
        in_specs=[any_] * 4,
        out_specs=[any_] * 5,
        out_shape=seq + own,
        input_output_aliases={0: 2},
        scratch_shapes=[pltpu.VMEM((dim,) + s, bf) for s in shapes] + [pltpu.VMEM((dim, n), bf) for n in (q_width, width, width)]
        + [pltpu.VMEM((2, rows, dim), bf), pltpu.VMEM((rows, dim), bf)] + [pltpu.VMEM((2, rows, width), bf)] * 2 + [pltpu.VMEM((rows, q_width), bf), pltpu.VMEM((rows, dim), bf)]
        + [sem((3,)), sem((2,)), sem((2,)), sem((2, 2))] + [sem((2, hops + 1, 2))] * 4 + [sem((2, 2)), sem((2, 2, hops + 1))],
        compiler_params=params(collective_id=1, has_side_effects=True),
        cost_estimate=pl.CostEstimate(flops=4 * rows * num_dev * dim * width, bytes_accessed=4 * dim * width, transcendentals=0),
        name="gather",
    )(x_all, w_query, w_key, w_value)


def causal_kernel(layer, num_dev, seq, q_ref, k_ref, v_ref, x_hbm, w_hbm, out_ref, o_s, w_s, x_s, upd_s, acc_s, top_s, tot_s, sem):
    g = pl.program_id(0)
    copies = [pltpu.make_async_copy(x_hbm, x_s, sem.at[0]), pltpu.make_async_copy(w_hbm.at[layer], w_s, sem.at[1])]

    @pl.when(g == 0)
    def _():
        for cp in copies:
            cp.start()

    lead = lax.axis_index("cp")
    trail = 2 * num_dev - 1 - lead
    tile = 4 * BLK
    lanes = tot_s.shape[-1]
    per = tile // BLK
    front = seq // 2 // tile
    num_trail = lax.div(trail + 1 + per - 1, per) - front
    factor = LOG2_E * BLK ** -0.5
    def scores(item):
        _, qrow, t, limit, h = item
        q = q_ref[pl.ds(qrow, BLK), h * BLK:(h + 1) * BLK]
        s = lax.dot_general(q, k_ref[pl.ds(t, tile), :], (((1,), (1,)), ((), ())), preferred_element_type=jnp.float32)
        if limit is not None:
            reach = lax.broadcasted_iota(jnp.int32, (BLK, 1), 0) + limit
            s = jnp.where(lax.broadcasted_iota(jnp.int32, s.shape, 1) <= reach, s, NEG_BIG)
        return s

    def finish(s, item):
        slot, _, t, _, h = item
        top = jnp.max(s, axis=-1, keepdims=True)
        e = jnp.exp2((s - top) * factor)
        tot_s[slot, h] = functools.reduce(jnp.add, [e[:, i * lanes:(i + 1) * lanes] for i in range(tile // lanes)])
        acc_s[slot, h] = jnp.dot(e.astype(jnp.bfloat16), v_ref[pl.ds(t, tile), :], preferred_element_type=jnp.float32)
        top_s[slot, h] = top

    items = []
    for j in range(front):
        chains = [(j, BLK, j * tile, None)]
        if j < 2:
            block, t = ((trail, front + num_trail - 1), (lead, front - num_trail))[j]
            t = pl.multiple_of(t * tile, tile)
            chains.append((front + j, (1 - j) * BLK, t, block * BLK - t))
        if j > 0:
            late = j < num_trail
            t = jnp.where(late, front + j - 1, j - num_trail) * tile
            chains.append((front + 1 + j, pl.multiple_of(jnp.where(late, BLK, 0), BLK), pl.multiple_of(t, tile), None))
        for chain in chains:
            items += [chain + (h,) for h in range(2)]
    ready = scores(items[0])
    for i, item in enumerate(items):
        now = ready
        if i + 1 < len(items):
            ready = scores(items[i + 1])
        finish(now, item)

    for h in range(2):
        cols = pl.ds(pl.multiple_of(g * 2 * BLK + h * BLK, BLK), BLK)
        shared = range(front + 2, 2 * front + 1)
        for i, slots in enumerate(([front + 1, *shared], [*range(front + 1), *shared])):
            tops = []
            for slot in slots:
                top = top_s[slot, h]
                if slot > front + 1:
                    late = slot - front - 1 < num_trail
                    top = jnp.where(late if i == 1 else jnp.logical_not(late), top, NEG_BIG)
                tops.append(top)
            new = functools.reduce(jnp.maximum, tops)
            acc = total = None
            for slot, top in zip(slots, tops):
                fix = jnp.exp2((top - new) * factor)
                a, b = acc_s[slot, h] * fix, tot_s[slot, h] * fix
                acc, total = (a, b) if acc is None else (acc + a, total + b)
            o_s[i * BLK:(i + 1) * BLK, cols] = (acc / jnp.sum(total, axis=-1, keepdims=True)).astype(jnp.bfloat16)

    @pl.when(g == pl.num_programs(0) - 1)
    def _():
        for cp in copies:
            cp.wait()
        output_rows(o_s, w_s, x_s, out_ref, upd_s)


def causal_layer(q, k_all, v_all, x, w_out, layer, num_dev):
    rows, dim = x.shape
    seq = k_all.shape[0]
    slots = 2 * (seq // 2 // (4 * BLK)) + 1
    kv = pl.BlockSpec((seq, BLK), lambda g: (0, g))
    any_ = pl.BlockSpec(memory_space=pl.ANY)
    return pl.pallas_call(
        functools.partial(causal_kernel, layer, num_dev, seq),
        grid=(k_all.shape[1] // BLK,),
        in_specs=[pl.BlockSpec((rows, 2 * BLK), lambda g: (0, g)), kv, kv, any_, any_],
        out_specs=pl.BlockSpec((rows, dim), lambda g: (0, 0)),
        scratch_shapes=[
            pltpu.VMEM(q.shape, jnp.bfloat16),
            pltpu.VMEM(w_out.shape[1:], jnp.bfloat16),
            pltpu.VMEM((rows, dim), jnp.bfloat16),
            pltpu.VMEM((rows, dim), jnp.float32),
            pltpu.VMEM((slots, 2, BLK, BLK), jnp.float32),
            pltpu.VMEM((slots, 2, BLK, 1), jnp.float32),
            pltpu.VMEM((slots, 2, BLK, 128), jnp.float32),
            pltpu.SemaphoreType.DMA((2,)),
        ],
        out_shape=jax.ShapeDtypeStruct((rows, dim), jnp.bfloat16),
        compiler_params=params(),
        cost_estimate=pl.CostEstimate(flops=30 * 10 ** 9, bytes_accessed=2 * w_out[0].size, transcendentals=0),
        name="causal",
    )(q, k_all, v_all, x, w_out)


def solution(mesh):
    num_dev = mesh.shape["cp"]

    def per_device(hidden, w_query, w_key, w_value, w_out):
        num_layers = w_query.shape[0]
        dim = hidden.shape[1]
        w_out = w_out.reshape(num_layers, -1, dim)
        last = num_layers - 1
        x = window_stack(hidden, w_query, w_key, w_value, w_out, last, num_dev)
        k_all, v_all, _, q, x_fin = gather_keys(x, w_query, w_key, w_value, last, last, num_dev)
        k_all, v_all = (t.reshape(-1, t.shape[-1]) for t in (k_all, v_all))
        return causal_layer(q, k_all, v_all, x_fin, w_out, last, num_dev)

    row_spec = P(("dp", "cp"), None)
    return jax.shard_map(per_device, mesh=mesh, in_specs=(row_spec, P(), P(), P(), P()), out_specs=row_spec, check_vma=False)
```

```python
import functools

import jax
import jax.numpy as jnp
from jax import lax
from jax.experimental import pallas as pl
from jax.experimental.pallas import tpu as pltpu
from jax.sharding import PartitionSpec as P

WINDOW = 1024
EPS_NORM = 1e-6
NEG_BIG = -1e30
LOG2_E = 1.4426950408889634
BLK = 256
VMEM_BYTES = 62 << 20
MESH = pl.DeviceIdType.MESH


def params(**kw):
    return pltpu.CompilerParams(vmem_limit_bytes=VMEM_BYTES, **kw)


def normed(rows):
    wide = rows.astype(jnp.float32)
    return (wide * lax.rsqrt(jnp.mean(wide * wide, axis=-1, keepdims=True) + EPS_NORM)).astype(jnp.bfloat16)


def output_rows(o_s, w_s, x_ref, out_ref, upd_s):
    rows, dim = x_ref.shape
    tile = 768

    @pl.loop(0, dim // tile)
    def _(s):
        cols = pl.ds(pl.multiple_of(s * tile, tile), tile)
        upd_s[:, cols] = jnp.dot(o_s[...], w_s[:, cols], preferred_element_type=jnp.float32)

    @pl.loop(0, rows // 16, unroll=16)
    def _(s):
        part = pl.ds(pl.multiple_of(s * 16, 16), 16)
        upd = upd_s[part, :]
        scale = lax.rsqrt(jnp.mean(upd * upd, axis=-1, keepdims=True) + EPS_NORM)
        out_ref[part, :] = (x_ref[part, :].astype(jnp.float32) + upd * scale).astype(jnp.bfloat16)


def scoped(name):
    def wrap(fn):
        def run(*args):
            with jax.named_scope(name):
                return fn(*args)

        return run

    return wrap


def stack_kernel(num_dev, num_layers, x_hbm, wq_hbm, wk_hbm, wv_hbm, wo_hbm, x_all,
                 xr, xn, kv, n_s, q_s, wq_s, wkv_s, wo_s, upd_s, stq, stk, stv,
                 g_send, g_recv, x_send, x_recv, h_send, h_recv, c_send, c_recv, h_free, c_free, xsem, qsem, ksem, vsem, wsem):
    blk, dim = n_s.shape
    width = wkv_s.shape[1] // 2
    heads = q_s.shape[2] // width
    head = BLK
    q_rows, kv_rows = stq.shape[1], stk.shape[1]
    q_ring, kv_ring = stq.shape[0], stk.shape[0]
    q_parts, kv_parts = dim // q_rows, dim // kv_rows
    me = lax.axis_index("cp")
    odd = lax.rem(me, 2)
    is_odd, is_even = odd == 1, odd == 0
    left, right = lax.rem(me + num_dev - 1, num_dev), lax.rem(me + 1, num_dev)

    other = jnp.where(is_odd, left, right)
    peers = (lax.rem(me + 2, num_dev), lax.rem(me + num_dev - 2, num_dev), other)
    sources = (peers[1], peers[0], other)

    def block(i):
        return pl.ds(pl.multiple_of(i * blk, blk), blk)

    def remote(src, dst, send, recv, dev):
        return pltpu.make_async_remote_copy(src_ref=src, dst_ref=dst, send_sem=send, recv_sem=recv, device_id={"cp": dev}, device_id_type=MESH)

    def x_copy(slot, s):
        return remote(xn.at[s], xr.at[slot, s], x_send.at[s], x_recv.at[slot, s], left)

    def g_copy(i, owner):
        return remote(xn.at[0], x_all.at[owner, block(0)], g_send.at[i], g_recv.at[i], peers[i])

    def keep(s):
        return pltpu.make_async_copy(xn.at[s], x_all.at[me, block(s)], xsem.at[s])

    def h_copy(s, j):
        cols = pl.ds(pl.multiple_of(j * width, width), width)
        return remote(kv.at[block(2 + s), cols], kv.at[block(s), cols], h_send.at[s, j], h_recv.at[s, j], right)

    def c_copy(s):
        return remote(kv.at[block(2 + s)], kv.at[block(4 + s)], c_send.at[s], c_recv.at[s], left)

    def signal(sem, dev):
        pl.semaphore_signal(sem, inc=1, device_id={"cp": dev}, device_id_type=MESH)

    def q_stage(layer, i):
        b = lax.rem(layer * q_parts + i, q_ring)
        return pltpu.make_async_copy(wq_hbm.at[layer, pl.ds(i * q_rows, q_rows)], stq.at[b], qsem.at[b])

    def kv_stage(layer, i):
        b = lax.rem(layer * kv_parts + i, kv_ring)
        rows = pl.ds(i * kv_rows, kv_rows)
        return (pltpu.make_async_copy(wk_hbm.at[layer, rows], stk.at[b], ksem.at[b]),
                pltpu.make_async_copy(wv_hbm.at[layer, rows], stv.at[b], vsem.at[b]))

    def kv_start(layer, i):
        for cp in kv_stage(layer, i):
            cp.start()

    def kv_wait(layer, i):
        for cp in kv_stage(layer, i):
            cp.wait()

    def kv_flat(layer, i):
        b = lax.rem(layer * kv_parts + i, kv_ring)
        rows = pl.ds(pl.multiple_of(i * kv_rows, 16), kv_rows)
        wkv_s[rows, :width] = stk[b].reshape(kv_rows, width)
        wkv_s[rows, width:] = stv[b].reshape(kv_rows, width)

    def q_flat(layer, i):
        b = lax.rem(layer * q_parts + i, q_ring)
        wq_s[pl.ds(pl.multiple_of(i * q_rows, 16), q_rows), :] = stq[b].reshape(q_rows, wq_s.shape[1])

    def kv_next(layer, i):
        @pl.when(i + kv_ring < kv_parts)
        def _():
            kv_start(layer, i + kv_ring)

    def q_next(layer, i):
        after = i + q_ring

        @pl.when(after < q_parts)
        def _():
            q_stage(layer, after).start()

        @pl.when((after >= q_parts) & (layer + 1 < num_layers))
        def _():
            q_stage(layer + 1, after - q_parts).start()

    def wo_copy(layer):
        return pltpu.make_async_copy(wo_hbm.at[layer], wo_s, wsem)

    def norm_into(ref):
        step = min(16, blk)

        @pl.loop(0, blk // step, unroll=blk // step)
        def _(i):
            part = pl.ds(pl.multiple_of(i * step, step), step)
            n_s[part, :] = normed(ref[part, :])

    def dot(w):
        return jnp.dot(n_s[...], w, preferred_element_type=jnp.float32).astype(jnp.bfloat16)

    def attend(s, span, start):
        window = WINDOW + blk
        rows = pl.ds(pl.multiple_of(s * blk + window - span, blk), span)
        factor = LOG2_E * head ** -0.5
        groups = width // head
        together = groups if span == window else 2
        qi = lax.broadcasted_iota(jnp.int32, (blk, blk), 0)
        ki = lax.broadcasted_iota(jnp.int32, (blk, blk), 1)

        def scores(item):
            sc = lax.dot_general(q_s[s, :, item[2]], kv[rows, item[0]], (((1,), (1,)), ((), ())), preferred_element_type=jnp.float32)
            last = jnp.where(ki <= qi, sc[:, span - blk:], NEG_BIG)
            if span == window:
                return jnp.concatenate([jnp.where(ki > qi, sc[:, :blk], NEG_BIG), sc[:, blk:span - blk], last], axis=1)
            mid = sc[:, :span - blk]
            pos = lax.broadcasted_iota(jnp.int32, mid.shape, 1)
            return jnp.concatenate([jnp.where(pos >= start - (window - span), mid, NEG_BIG), last], axis=1)

        def finish(sc, item):
            top = jnp.max(sc, axis=-1, keepdims=True)
            e = jnp.exp2((sc - top) * factor)
            total = jnp.sum(e, axis=-1, keepdims=True)
            acc = jnp.dot(e.astype(jnp.bfloat16), kv[rows, item[1]], preferred_element_type=jnp.float32)
            return (acc / total).astype(jnp.bfloat16)

        def some(first):
            items = []
            for u in range(together):
                g = first + u
                for h in range(heads):
                    offsets = (g * head, width + g * head, (g * heads + h) * head)
                    items.append(tuple(pl.ds(o if isinstance(o, int) else pl.multiple_of(o, head), head) for o in offsets))
            ahead = scores(items[0])
            for k, item in enumerate(items):
                now = ahead
                if k + 1 < len(items):
                    ahead = scores(items[k + 1])
                q_s[s, :, item[2]] = finish(now, item)

        if together == groups:
            some(0)
        else:
            @pl.loop(0, groups // together)
            def _(i):
                some(i * together)

    tile = width
    loads = [pltpu.make_async_copy(x_hbm.at[block(s)], xn.at[s], xsem.at[s]) for s in range(2)]
    for cp in loads:
        cp.start()
    for i in range(kv_ring):
        kv_start(0, i)
    for i in range(q_ring):
        q_stage(0, i).start()
    barrier = pltpu.get_barrier_semaphore()
    for dev in (left, right) + peers[:2]:
        signal(barrier, dev)
    pl.semaphore_wait(barrier, 4)
    for s in range(2):
        loads[s].wait()
        x_copy(0, s).start()

    @pl.loop(0, kv_parts)
    def _(i):
        kv_wait(0, i)
        kv_flat(0, i)
        kv_next(0, i)

    @pl.loop(0, num_layers)
    def _(layer):
        slot = lax.rem(layer, 2)
        more = layer + 1 < num_layers
        chunk = lax.rem(me + layer + 1, num_dev)

        @pl.when(layer > 0)
        def _():
            for s in range(2):
                for j in range(2):
                    h_copy(s, j).wait_send()

            @pl.when(is_odd)
            def _():
                for s in range(2):
                    c_copy(s).wait_send()

        @pl.loop(0, 2)
        def _(s):
            with jax.named_scope("own_norm"):
                norm_into(xn.at[s])

            @pl.loop(0, 2)
            @scoped("own")
            def _(j):
                cols = pl.ds(pl.multiple_of(j * tile, tile), tile)
                kv[block(2 + s), cols] = dot(wkv_s[:, cols])

                @pl.when((layer > 0) & (s == 0) & (j == 0))
                def _():
                    pl.semaphore_wait(h_free, 1)

                    @pl.when(is_odd)
                    def _():
                        pl.semaphore_wait(c_free, 1)

                h_copy(s, j).start()

            @pl.when(is_odd)
            def _():
                c_copy(s).start()

        @pl.loop(0, q_parts)
        @scoped("q_lay")
        def _(i):
            q_stage(layer, i).wait()
            q_flat(layer, i)
            q_next(layer, i)

        wo_copy(layer).start()

        @pl.when(more)
        def _():
            for i in range(kv_ring):
                kv_start(layer + 1, i)

        @pl.loop(0, 2)
        def _(s):
            @pl.loop(jnp.where(is_odd, s, 2 * s), jnp.where(is_odd, s + 1, 2))
            def _(t):
                with jax.named_scope("x_wait"):
                    x_copy(slot, t).wait_recv()
                with jax.named_scope("norm"):
                    norm_into(xr.at[slot, t])

                @pl.loop(0, 2)
                @scoped("query")
                def _(j):
                    cols = pl.ds(pl.multiple_of(j * tile, tile), tile)
                    q_s[t, :, cols] = dot(wq_s[:, cols])

                @pl.when(is_odd)
                def _():
                    @pl.loop(0, 2)
                    @scoped("keys")
                    def _(j):
                        cols = pl.ds(pl.multiple_of(j * tile, tile), tile)
                        kv[block(4 + t), cols] = dot(wkv_s[:, cols])

            @pl.when((s == 0) & more & is_even)
            def _():
                @pl.loop(0, kv_parts)
                def _(i):
                    kv_wait(layer + 1, i)
                    kv_flat(layer + 1, i)
                    kv_next(layer + 1, i)

            @pl.when(s == 0)
            @scoped("h_wait")
            def _():
                for i in range(2):
                    for j in range(2):
                        h_copy(i, j).wait_recv()

            @pl.when(is_even)
            @scoped("c_wait")
            def _():
                c_copy(s).wait_recv()

            for first, cond in ((2, chunk >= 2), (1, chunk == 1), (0, chunk == 0)):
                @pl.when(cond)
                @scoped("attend")
                def _():
                    attend(s, (2 * first + 1) * blk if first == 2 else (2 * first + 2) * blk, WINDOW - s * blk - first * 2 * blk)

            @pl.when((s == 1) & more)
            def _():
                signal(h_free, left)

                @pl.when(is_even)
                def _():
                    signal(c_free, right)

            out_tiles = 3
            out_tile = dim // out_tiles

            @pl.when(s == 0)
            def _():
                wo_copy(layer).wait()

            def out_dot(j):
                cols = pl.ds(pl.multiple_of(j * out_tile, out_tile), out_tile)
                upd_s[:, cols] = jnp.dot(q_s[s], wo_s[:, cols], preferred_element_type=jnp.float32)

            relay = (s == 1) & more & is_odd

            @pl.when(relay)
            def _():
                @pl.loop(0, out_tiles)
                @scoped("out_lay")
                def _(j):
                    per = kv_parts // out_tiles
                    for t in range(per):
                        kv_wait(layer + 1, j * per + t)
                        kv_flat(layer + 1, j * per + t)
                        kv_next(layer + 1, j * per + t)
                    out_dot(j)

            @pl.when(jnp.logical_not(relay))
            def _():
                @pl.loop(0, out_tiles)
                @scoped("out")
                def _(j):
                    out_dot(j)

            with jax.named_scope("x_sent"):
                x_copy(slot, s).wait_send()
            step = min(16, blk)

            @pl.loop(0, blk // step, unroll=blk // step)
            def _(i):
                part = pl.ds(pl.multiple_of(i * step, step), step)
                upd = upd_s[part, :]
                scale = lax.rsqrt(jnp.mean(upd * upd, axis=-1, keepdims=True) + EPS_NORM)
                xn[s, part, :] = (xr[slot, s, part, :].astype(jnp.float32) + upd * scale).astype(jnp.bfloat16)

            @pl.when(more)
            def _():
                x_copy(1 - slot, s).start()

            @pl.when(jnp.logical_not(more))
            def _():
                keep(s).start()

                @pl.when(s == 0)
                def _():
                    for i in range(3):
                        g_copy(i, me).start()

    for s in range(2):
        for j in range(2):
            h_copy(s, j).wait_send()
        keep(s).wait()

    @pl.when(is_odd)
    def _():
        for s in range(2):
            c_copy(s).wait_send()

    for i in range(3):
        g_copy(i, me).wait_send()
        g_copy(i, sources[i]).wait_recv()


def window_stack(x, w_query, w_key, w_value, w_out, num_layers, num_dev):
    rows, dim = x.shape
    blk = rows // 2
    q_heads, head = w_query.shape[2:]
    kv_heads = w_key.shape[2]
    q_width, width = q_heads * head, kv_heads * head
    q_rows, q_ring, kv_rows, kv_ring = dim // 8, 4, dim // 9, 4
    any_ = pl.BlockSpec(memory_space=pl.ANY)
    bf = jnp.bfloat16
    dma, regular = pltpu.SemaphoreType.DMA, pltpu.SemaphoreType.REGULAR
    return pl.pallas_call(
        functools.partial(stack_kernel, num_dev, num_layers),
        in_specs=[any_] * 5,
        out_specs=any_,
        out_shape=jax.ShapeDtypeStruct((num_dev, rows, dim), bf),
        scratch_shapes=[
            pltpu.VMEM((2, 2, blk, dim), bf),
            pltpu.VMEM((2, blk, dim), bf),
            pltpu.VMEM((6 * blk, 2 * width), bf),
            pltpu.VMEM((blk, dim), bf),
            pltpu.VMEM((2, blk, q_width), bf),
            pltpu.VMEM((dim, q_width), bf),
            pltpu.VMEM((dim, 2 * width), bf),
            pltpu.VMEM((q_width, dim), bf),
            pltpu.VMEM((blk, dim), jnp.float32),
            pltpu.VMEM((q_ring, q_rows, q_heads, head), bf),
            pltpu.VMEM((kv_ring, kv_rows, kv_heads, head), bf),
            pltpu.VMEM((kv_ring, kv_rows, kv_heads, head), bf),
            dma((3,)), dma((3,)), dma((2,)), dma((2, 2)), dma((2, 2)), dma((2, 2)), dma((2,)), dma((2,)),
            regular, regular, dma((2,)), dma((q_ring,)), dma((kv_ring,)), dma((kv_ring,)), dma,
        ],
        compiler_params=pltpu.CompilerParams(vmem_limit_bytes=67043328, collective_id=2, has_side_effects=True),
        cost_estimate=pl.CostEstimate(flops=num_layers * 20 * 10 ** 9, bytes_accessed=num_layers * 28 * 10 ** 6, transcendentals=0),
        name="stack",
    )(x, w_query, w_key, w_value, w_out)


def norm_rows(src, dst):
    rows = src.shape[0]
    step = min(16, rows)

    @pl.loop(0, rows // step, unroll=min(16, rows // step))
    def _(i):
        part = pl.ds(pl.multiple_of(i * step, step), step)
        dst[part, :] = normed(src[part, :])


def gather_kernel(num_dev, layer, shift, x_in, wq_hbm, wk_hbm, wv_hbm, k_all, v_all, x_all, q_hbm, x_fin,
                  wq_st, wk_st, wv_st, wq_s, wk_s, wv_s, x_s, n_s, k_s, v_s, q_s, f_s, wsem, fsem, lsem, ssem, send, recv, psend, precv, csend, crecv):
    _, rows, dim = x_s.shape
    half = rows // 2
    me = lax.axis_index("cp")
    other = me + 1 - 2 * lax.rem(me, 2)
    near = (lax.rem(me + 2, num_dev), lax.rem(me + num_dev - 2, num_dev))
    hops = num_dev // 4

    def wrap(v):
        return lax.rem(v + 4 * num_dev, num_dev)

    def owner(dev, way, hop):
        if isinstance(way, int):
            return wrap(dev - 2 * hop) if way == 0 else wrap(dev + 2 * hop)
        return wrap(dev + jnp.where(way == 0, -2, 2) * hop)

    def piece(dev, h):
        return x_all.at[dev, pl.ds(h * half, half)]

    def link(way, hop, h):
        ref = piece(owner(me, way, hop - 1), h)
        return pltpu.make_async_remote_copy(src_ref=ref, dst_ref=ref, send_sem=send.at[way, hop, h], recv_sem=recv.at[way, hop, h],
                                            device_id={"cp": near[way]}, device_id_type=MESH)

    def landed(way, hop, h):
        ref = piece(owner(me, way, hop), h)
        return pltpu.make_async_remote_copy(src_ref=ref, dst_ref=ref, send_sem=send.at[way, hop, h], recv_sem=recv.at[way, hop, h],
                                            device_id={"cp": near[way]}, device_id_type=MESH)

    def across(way, hop, h, dev):
        ref = piece(owner(dev, way, hop), h)
        return pltpu.make_async_remote_copy(src_ref=ref, dst_ref=ref, send_sem=psend.at[way, hop, h], recv_sem=precv.at[way, hop, h],
                                            device_id={"cp": other}, device_id_type=MESH)

    crossings = [(0, 0, 1)] + [(way, hop, h) for hop in range(1, hops + 1) for way in range(2) for h in range(2) if hop < hops or way == h]

    def share(i, a, hop, chunk):
        src, dst = ((k_s, k_all), (v_s, v_all))[i]
        return pltpu.make_async_remote_copy(src_ref=src.at[a], dst_ref=dst.at[chunk], send_sem=csend.at[i, a], recv_sem=crecv.at[i, a, hop],
                                            device_id={"cp": other}, device_id_type=MESH)

    def kept(i):
        block = jnp.where(i == 0, me, 2 * num_dev - 1 - me)
        return wrap(lax.div(block, 2) - shift), block

    def early(i):
        return lax.div(kept(i)[0], 2) != lax.rem(lax.div(me, 2) + hops, num_dev // 2)

    def final(i):
        src, block = kept(i)
        return pltpu.make_async_copy(piece(src, lax.rem(block, 2)), f_s.at[pl.ds(i * half, half)], fsem.at[i])

    def queries(i):
        part = pl.ds(pl.multiple_of(i * half, half), half)
        final(i).wait()
        norm_rows(f_s.at[part], n_s.at[pl.ds(0, half)])
        with jax.named_scope("query"):
            q_s[part, :] = jnp.dot(n_s[:half], wq_s[...], preferred_element_type=jnp.float32).astype(jnp.bfloat16)

    wcopies = [pltpu.make_async_copy(w.at[layer], st, wsem.at[i]) for i, (w, st) in enumerate(((wk_hbm, wk_st), (wv_hbm, wv_st), (wq_hbm, wq_st)))]
    for cp in wcopies:
        cp.start()
    barrier = pltpu.get_barrier_semaphore()
    for dev in near + (other,):
        pl.semaphore_signal(barrier, inc=1, device_id={"cp": dev}, device_id_type=MESH)
    pl.semaphore_wait(barrier, 3)
    for way in range(2):
        link(way, 1, 1).start()
    across(0, 0, 1, me).start()
    for way in range(2):
        link(way, 2, 0).start()
        across(way, 1, 0, me).start()
    for cp in wcopies:
        cp.wait()
    step_rows = 256

    @pl.loop(0, dim // step_rows)
    def _(s):
        part = pl.ds(pl.multiple_of(s * step_rows, step_rows), step_rows)
        wk_s[part, :] = wk_st[part].reshape(step_rows, -1)
        wv_s[part, :] = wv_st[part].reshape(step_rows, -1)
        wq_s[part, :] = wq_st[part].reshape(step_rows, -1)

    @pl.loop(0, hops + 1)
    def _(hop):
        @pl.when(hop == hops)
        def _():
            for way, far, h in crossings:
                if far < hops:
                    across(way, far, h, other).wait_recv()
            for i in range(2):
                pl.when(early(i))(final(i).start)

            @pl.loop(0, 2)
            def _(i):
                @pl.when(early(i))
                def _():
                    queries(i)

        for h in range(2):
            for way in range(2):
                last_ok = way == h

                def arrive():
                    with jax.named_scope("land"):
                        landed(way, hop, h).wait_recv()
                    if last_ok:
                        @pl.when(hop < hops)
                        def _():
                            link(way, hop + 1, h).start()
                    else:
                        @pl.when(hop < hops - 1)
                        def _():
                            link(way, hop + 1, h).start()
                    across(way, hop, h, me).start()

                first_hop = 2 - h
                if last_ok:
                    pl.when(hop >= first_hop)(arrive)
                else:
                    pl.when((hop >= first_hop) & (hop < hops))(arrive)

        whole = (hop > 0) & (hop < hops)
        count = jnp.where(whole, 2, 1)

        def source(a):
            return wrap(me + jnp.where(a == 0, -2, 2) * hop)

        def load(a):
            return pltpu.make_async_copy(x_all.at[source(a)], x_s.at[a], lsem.at[a])

        load(0).start()

        @pl.loop(0, count)
        def _(a):
            with jax.named_scope("load"):
                load(a).wait()

            @pl.when(a + 1 < count)
            def _():
                load(a + 1).start()

            with jax.named_scope("norm"):
                norm_rows(x_s.at[a], n_s)
            chunk = wrap(source(a) + shift)

            def keep(i):
                src, dst = ((k_s, k_all), (v_s, v_all))[i]
                return pltpu.make_async_copy(src.at[a], dst.at[chunk], ssem.at[i, a])

            with jax.named_scope("keys"):
                k_s[a] = jnp.dot(n_s[...], wk_s[...], preferred_element_type=jnp.float32).astype(jnp.bfloat16)
            keep(0).start()
            share(0, a, hop, chunk).start()

            @pl.when(hop == hops)
            @scoped("cross")
            def _():
                for way in range(2):
                    across(way, hops, way, other).wait_recv()
                for i in range(2):
                    pl.when(jnp.logical_not(early(i)))(final(i).start)

            with jax.named_scope("keys"):
                v_s[a] = jnp.dot(n_s[...], wv_s[...], preferred_element_type=jnp.float32).astype(jnp.bfloat16)
            keep(1).start()
            share(1, a, hop, chunk).start()

        @pl.loop(0, count)
        def _(a):
            for i in range(2):
                src, dst = ((k_s, k_all), (v_s, v_all))[i]
                pltpu.make_async_copy(src.at[a], dst.at[wrap(source(a) + shift)], ssem.at[i, a]).wait()

                @pl.when(hop < hops)
                @scoped("shared")
                def _():
                    share(i, a, hop, wrap(source(a) + shift)).wait_send()

    @pl.loop(0, 2)
    def _(i):
        @pl.when(jnp.logical_not(early(i)))
        def _():
            queries(i)

    keep = pltpu.make_async_copy(f_s, x_fin, lsem.at[0])
    keep.start()
    last = pltpu.make_async_copy(q_s, q_hbm, lsem.at[1])
    last.start()
    last.wait()
    keep.wait()
    for i in range(2):
        share(i, 0, hops, wrap(me + shift)).wait_send()
        for hop in range(hops + 1):
            for way in range(2 if 0 < hop < hops else 1):
                share(i, way, hop, wrap(owner(other, way, hop) + shift)).wait_recv()
    for way, hop, h in crossings:
        across(way, hop, h, me).wait_send()
        if hop + h > 1:
            link(way, hop, h).wait_send()


def gather_keys(x_all, w_query, w_key, w_value, layer, shift, num_dev):
    _, rows, dim = x_all.shape
    shapes = [w.shape[2:] for w in (w_query, w_key, w_value)]
    q_width, width = (h * e for h, e in shapes[:2])
    hops = num_dev // 4
    any_ = pl.BlockSpec(memory_space=pl.ANY)
    bf = jnp.bfloat16
    sem = pltpu.SemaphoreType.DMA
    seq = [jax.ShapeDtypeStruct((num_dev, rows, n), bf) for n in (width, width, dim)]
    own = [jax.ShapeDtypeStruct((rows, n), bf) for n in (q_width, dim)]
    return pl.pallas_call(
        functools.partial(gather_kernel, num_dev, layer, shift),
        in_specs=[any_] * 4,
        out_specs=[any_] * 5,
        out_shape=seq + own,
        input_output_aliases={0: 2},
        scratch_shapes=[pltpu.VMEM((dim,) + s, bf) for s in shapes] + [pltpu.VMEM((dim, n), bf) for n in (q_width, width, width)]
        + [pltpu.VMEM((2, rows, dim), bf), pltpu.VMEM((rows, dim), bf)] + [pltpu.VMEM((2, rows, width), bf)] * 2 + [pltpu.VMEM((rows, q_width), bf), pltpu.VMEM((rows, dim), bf)]
        + [sem((3,)), sem((2,)), sem((2,)), sem((2, 2))] + [sem((2, hops + 1, 2))] * 4 + [sem((2, 2)), sem((2, 2, hops + 1))],
        compiler_params=params(collective_id=1, has_side_effects=True),
        cost_estimate=pl.CostEstimate(flops=4 * rows * num_dev * dim * width, bytes_accessed=4 * dim * width, transcendentals=0),
        name="gather",
    )(x_all, w_query, w_key, w_value)


def causal_kernel(layer, num_dev, seq, q_ref, k_ref, v_ref, x_hbm, w_hbm, out_ref, o_s, w_s, x_s, upd_s, acc_s, top_s, tot_s, sem):
    g = pl.program_id(0)
    copies = [pltpu.make_async_copy(x_hbm, x_s, sem.at[0]), pltpu.make_async_copy(w_hbm.at[layer], w_s, sem.at[1])]

    @pl.when(g == 0)
    def _():
        for cp in copies:
            cp.start()

    lead = lax.axis_index("cp")
    trail = 2 * num_dev - 1 - lead
    tile = 4 * BLK
    lanes = tot_s.shape[-1]
    per = tile // BLK
    front = seq // 2 // tile
    num_trail = lax.div(trail + 1 + per - 1, per) - front
    factor = LOG2_E * BLK ** -0.5
    def scores(item):
        _, qrow, t, limit, h = item
        q = q_ref[pl.ds(qrow, BLK), h * BLK:(h + 1) * BLK]
        s = lax.dot_general(q, k_ref[pl.ds(t, tile), :], (((1,), (1,)), ((), ())), preferred_element_type=jnp.float32)
        if limit is not None:
            reach = lax.broadcasted_iota(jnp.int32, (BLK, 1), 0) + limit
            s = jnp.where(lax.broadcasted_iota(jnp.int32, s.shape, 1) <= reach, s, NEG_BIG)
        return s

    def finish(s, item):
        slot, _, t, _, h = item
        top = jnp.max(s, axis=-1, keepdims=True)
        e = jnp.exp2((s - top) * factor)
        tot_s[slot, h] = functools.reduce(jnp.add, [e[:, i * lanes:(i + 1) * lanes] for i in range(tile // lanes)])
        acc_s[slot, h] = jnp.dot(e.astype(jnp.bfloat16), v_ref[pl.ds(t, tile), :], preferred_element_type=jnp.float32)
        top_s[slot, h] = top

    items = []
    for j in range(front):
        chains = [(j, BLK, j * tile, None)]
        if j < 2:
            block, t = ((trail, front + num_trail - 1), (lead, front - num_trail))[j]
            t = pl.multiple_of(t * tile, tile)
            chains.append((front + j, (1 - j) * BLK, t, block * BLK - t))
        if j > 0:
            late = j < num_trail
            t = jnp.where(late, front + j - 1, j - num_trail) * tile
            chains.append((front + 1 + j, pl.multiple_of(jnp.where(late, BLK, 0), BLK), pl.multiple_of(t, tile), None))
        for chain in chains:
            items += [chain + (h,) for h in range(2)]
    ready = scores(items[0])
    for i, item in enumerate(items):
        now = ready
        if i + 1 < len(items):
            ready = scores(items[i + 1])
        finish(now, item)

    for h in range(2):
        cols = pl.ds(pl.multiple_of(g * 2 * BLK + h * BLK, BLK), BLK)
        shared = range(front + 2, 2 * front + 1)
        for i, slots in enumerate(([front + 1, *shared], [*range(front + 1), *shared])):
            tops = []
            for slot in slots:
                top = top_s[slot, h]
                if slot > front + 1:
                    late = slot - front - 1 < num_trail
                    top = jnp.where(late if i == 1 else jnp.logical_not(late), top, NEG_BIG)
                tops.append(top)
            new = functools.reduce(jnp.maximum, tops)
            acc = total = None
            for slot, top in zip(slots, tops):
                fix = jnp.exp2((top - new) * factor)
                a, b = acc_s[slot, h] * fix, tot_s[slot, h] * fix
                acc, total = (a, b) if acc is None else (acc + a, total + b)
            o_s[i * BLK:(i + 1) * BLK, cols] = (acc / jnp.sum(total, axis=-1, keepdims=True)).astype(jnp.bfloat16)

    @pl.when(g == pl.num_programs(0) - 1)
    def _():
        for cp in copies:
            cp.wait()
        output_rows(o_s, w_s, x_s, out_ref, upd_s)


def causal_layer(q, k_all, v_all, x, w_out, layer, num_dev):
    rows, dim = x.shape
    seq = k_all.shape[0]
    slots = 2 * (seq // 2 // (4 * BLK)) + 1
    kv = pl.BlockSpec((seq, BLK), lambda g: (0, g))
    any_ = pl.BlockSpec(memory_space=pl.ANY)
    return pl.pallas_call(
        functools.partial(causal_kernel, layer, num_dev, seq),
        grid=(k_all.shape[1] // BLK,),
        in_specs=[pl.BlockSpec((rows, 2 * BLK), lambda g: (0, g)), kv, kv, any_, any_],
        out_specs=pl.BlockSpec((rows, dim), lambda g: (0, 0)),
        scratch_shapes=[
            pltpu.VMEM(q.shape, jnp.bfloat16),
            pltpu.VMEM(w_out.shape[1:], jnp.bfloat16),
            pltpu.VMEM((rows, dim), jnp.bfloat16),
            pltpu.VMEM((rows, dim), jnp.float32),
            pltpu.VMEM((slots, 2, BLK, BLK), jnp.float32),
            pltpu.VMEM((slots, 2, BLK, 1), jnp.float32),
            pltpu.VMEM((slots, 2, BLK, 128), jnp.float32),
            pltpu.SemaphoreType.DMA((2,)),
        ],
        out_shape=jax.ShapeDtypeStruct((rows, dim), jnp.bfloat16),
        compiler_params=params(),
        cost_estimate=pl.CostEstimate(flops=30 * 10 ** 9, bytes_accessed=2 * w_out[0].size, transcendentals=0),
        name="causal",
    )(q, k_all, v_all, x, w_out)


def solution(mesh):
    num_dev = mesh.shape["cp"]

    def per_device(hidden, w_query, w_key, w_value, w_out):
        num_layers = w_query.shape[0]
        dim = hidden.shape[1]
        w_out = w_out.reshape(num_layers, -1, dim)
        last = num_layers - 1
        x = window_stack(hidden, w_query, w_key, w_value, w_out, last, num_dev)
        k_all, v_all, _, q, x_fin = gather_keys(x, w_query, w_key, w_value, last, last, num_dev)
        k_all, v_all = (t.reshape(-1, t.shape[-1]) for t in (k_all, v_all))
        return causal_layer(q, k_all, v_all, x_fin, w_out, last, num_dev)

    row_spec = P(("dp", "cp"), None)
    return jax.shard_map(per_device, mesh=mesh, in_specs=(row_spec, P(), P(), P(), P()), out_specs=row_spec, check_vma=False)
```
